128 devices in a mesh: head: 32 (over z, y, x_hi), kdim: 4 (over x_lo, core).
Axes of the slice: x: 4 (x_hi: 2, x_lo: 2; x = x_hi * 2 + x_lo), y: 4, z: 4, core: 2. Of those that a mesh axis runs over, the one named last changes fastest.
Arguments:
- hidden: bfloat16 [3, 1024, 8192], P(None, None, 'kdim'), may hold values from -6 to 6
- joined_weight: bfloat16 [3, 8192, 10240], P(None, 'kdim', 'head'), may hold values from -0.0625 to 0.0625
- src_block: int32 [8], replicated, may hold values from 0 to 7, each once
- group_map: int32 [8], replicated, may hold values from 0 to 7, each once
- q_slot: int32 [64], replicated, may hold values from 0 to 7, as said below
Outputs:
- qkv: float32 [3, 1024, 16384], P(None, 'kdim', 'head')
The draws below stay inside these ranges and needn't reach their ends.
Inputs may be any that keep to these rules, and one draw needn't show every extreme that they name: `q_slot`: for every key head g, the entries g * 8 to g * 8 + 7 are a permutation of 0 to 7.
All inputs are finite; a program needn't handle non-finite values.
Results may differ from the reference program's by a relative error of at most 0.0003.
Values may be sent and summed in bfloat16 or wider, within the bound.
No kernel may reach another device: no remote copies, remote signals or barrier semaphores. Data moves between devices by JAX's collectives and lax.ppermute only.
A program may use at most 64 MiB of HBM per device.

```python
import jax
import jax.numpy as jnp

D = 8192
HEAD_DIM = 128
Q_HEADS = 64
KV_HEADS = 8
LAYERS = 3
ROWS = 1024
GROUP = 8
BLOCK = 1280
JOINED = 10240
N_HEAD = 32


def draw_q_slot(key, part):
    group_keys = jax.random.split(jax.random.fold_in(key, 17), KV_HEADS)
    perms = jax.vmap(lambda one_key: jax.random.permutation(one_key, Q_HEADS // KV_HEADS))(group_keys)
    return perms.reshape(-1).astype(jnp.int32)


def block_scale(rng, extent, shards, least, largest):
    loudness, own = 1.0, jax.random.fold_in(rng, 6)
    for position, blocks in shards:
        steps = jnp.exp(jax.random.uniform(jax.random.fold_in(own, position), (blocks,), jnp.float32, least / len(shards), largest / len(shards)))
        loudness = loudness * jnp.repeat(steps, extent[position] // blocks).reshape([-1 if axis == position else 1 for axis in range(len(extent))])
    return loudness


def centred(stream_key, shape, width, bound, cuts=(), kind=jnp.bfloat16):
    values = jax.random.normal(stream_key, shape, jnp.float32) * width
    if len(cuts) > 0:
        values = block_scale(stream_key, shape, cuts, -0.22, 0.18) * values
    return jnp.clip(values, min=-bound, max=bound).astype(kind)


def setup_inputs(seed: int = 0) -> dict:
    seeds = jax.random.split(jax.random.key(seed), 6)
    hidden = centred(seeds[0], (LAYERS, ROWS, D), 1.0, 6.0, ((2, 4),))
    joined_weight = centred(seeds[1], (LAYERS, D, JOINED), D ** -0.5, 0.0625, ((1, 4), (2, 32)))
    src_block = jax.random.permutation(seeds[2], KV_HEADS).astype(jnp.int32)
    group_map = jax.random.permutation(seeds[3], KV_HEADS).astype(jnp.int32)
    q_slot = draw_q_slot(jax.random.fold_in(seeds[5], 71), 0)
    return dict(hidden=hidden, joined_weight=joined_weight, src_block=src_block, group_map=group_map, q_slot=q_slot)


def build_table(src_block, group_map, q_slot):
    group_devs = N_HEAD // KV_HEADS
    slot_count = Q_HEADS // N_HEAD
    devices = jnp.arange(N_HEAD, dtype=jnp.int32)
    group_ids = devices // group_devs
    quarter = devices % group_devs
    rank_ids = jnp.arange(KV_HEADS, dtype=jnp.int32)
    owner = jnp.sum(rank_ids[None, :] * (group_map[None, :] == group_ids[:, None]), axis=1).astype(jnp.int32)
    block_start = (jnp.sum(src_block[None, :] * (rank_ids[None, :] == owner[:, None]), axis=1) * BLOCK).astype(jnp.int32)
    members = (owner[:, None] * GROUP + jnp.arange(GROUP, dtype=jnp.int32)[None, :]).astype(jnp.int32)
    member_slot = q_slot[members]
    positions = quarter[:, None] * slot_count + jnp.arange(slot_count, dtype=jnp.int32)[None, :]
    local_head = jnp.sum(jnp.arange(GROUP, dtype=jnp.int32)[None, None, :] * (member_slot[:, None, :] == positions[:, :, None]), axis=2).astype(jnp.int32)
    q_cols = block_start[:, None, None] + local_head[:, :, None] * HEAD_DIM + jnp.arange(HEAD_DIM, dtype=jnp.int32)[None, None, :]
    kv_cols = block_start[:, None] + GROUP * HEAD_DIM + jnp.arange(2 * HEAD_DIM, dtype=jnp.int32)[None, :]
    columns = jnp.concatenate([q_cols.reshape(N_HEAD, slot_count * HEAD_DIM), kv_cols], axis=1)
    return columns.reshape(-1).astype(jnp.int32)


def reference(hidden, joined_weight, src_block, group_map, q_slot):
    columns = build_table(src_block, group_map, q_slot)
    results = []
    for layer in range(LAYERS):
        full = jnp.dot(hidden[layer], joined_weight[layer], preferred_element_type=jnp.float32)
        results.append(full[:, columns])
    return jnp.stack(results, axis=0)
```

```python
import jax
import jax.numpy as jnp
from jax import lax
from jax.experimental import pallas as pl
from jax.experimental.pallas import tpu as pltpu
from jax.sharding import Mesh, PartitionSpec as P

LAYERS = 3
ROWS = 1024
SLICE = 256
LANES = 128
WIDTH = 320
PADDED = 384
HEADS = 32
GROUP_DEVS = 4
KV_HEADS = 8
GROUP = 8
CODES = 256.0
TOP = 32700.0


def codes_of(amax):
    return jnp.ceil(CODES * jnp.log2(jnp.maximum(amax, 1e-30) * (1.0 / TOP))).astype(jnp.int32)


def scale_of(code):
    return jnp.exp2(code.astype(jnp.float32) * (1.0 / CODES))


def inverse_scale_of(code):
    return jnp.exp2(code.astype(jnp.float32) * (-1.0 / CODES))


def whole(x, inverse):
    return jnp.round(x * inverse).astype(jnp.int32)


def packed(low, high):
    return (low & 0xFFFF) | (high << 16)


def low_of(words):
    return (words << 16) >> 16


def high_of(words):
    return words >> 16


def row_max(*tiles):
    top = jnp.abs(tiles[0])
    for tile in tiles[1:]:
        top = jnp.maximum(top, jnp.abs(tile))
    return jnp.max(top, axis=1, keepdims=True)


def lanes_of(shape):
    return lax.broadcasted_iota(jnp.int32, shape, 1)


def product_kernel(place, hidden, weight, out):
    value = lax.dot_general(
        hidden[0], weight[0], (((1,), (1,)), ((), ())), preferred_element_type=jnp.float32
    )
    odd = place[1]

    @pl.when(odd == 0)
    def _():
        out[0, 0, :, :WIDTH] = value
        out[0, 0, :, WIDTH:] = jnp.zeros((SLICE, PADDED - WIDTH), jnp.float32)

    @pl.when(odd == 1)
    def _():
        out[0, 0, :, :256] = value[:, 64:]
        out[0, 0, :, 256:320] = jnp.zeros((SLICE, 64), jnp.float32)
        out[0, 0, :, 320:] = value[:, :64]


def product(place, hidden, weight, other):
    def token_block(l, x, place):
        core = 1 - place[0] if other else place[0]
        return (l, 2 * x + core, 0)

    return pl.pallas_call(
        product_kernel,
        grid_spec=pltpu.PrefetchScalarGridSpec(
            num_scalar_prefetch=1,
            grid=(LAYERS, 2),
            in_specs=[
                pl.BlockSpec((1, SLICE, 2048), token_block),
                pl.BlockSpec((1, WIDTH, 2048), lambda l, x, place: (l, 0, 0)),
            ],
            out_specs=pl.BlockSpec((1, 1, SLICE, PADDED), lambda l, x, place: (l, x, 0, 0)),
        ),
        out_shape=jax.ShapeDtypeStruct((LAYERS, 2, SLICE, PADDED), jnp.float32),
        cost_estimate=pl.CostEstimate(
            flops=LAYERS * 512 * 2048 * WIDTH * 2, bytes_accessed=12_000_000, transcendentals=0
        ),
        name="product",
    )(place, hidden, weight)


PACK_HEADS = 8


def pack_kernel(place, mine, theirs, out):
    odd = place[1]
    lane = lanes_of((8, LANES))
    spare = (lane >= 64) != (odd == 1)
    slot = lane & 63
    for i in range(PACK_HEADS):
        rows = slice(8 * i, 8 * i + 8)
        rest, codes = [], []
        for l in range(LAYERS):
            tiles = []
            for t in range(3):
                cols = slice(LANES * t, LANES * t + LANES)
                tiles.append(mine[l, 0, rows, cols] + theirs[l, 0, rows, cols])
            code = codes_of(row_max(*tiles))
            inverse = inverse_scale_of(code)
            a, b, c = [whole(tile, inverse) for tile in tiles]
            out[0, i, 8 * l : 8 * l + 8, :] = packed(a, b)
            rest.append(c)
            codes.append(code)
        code = jnp.where(slot == 0, codes[0], jnp.where(slot == 1, codes[1], codes[2]))
        low = rest[0] + pltpu.roll(rest[1], 64, 1)
        high = jnp.where(spare, code, rest[2])
        out[0, i, 24:32, :] = packed(low, high)


def pack(place, mine, theirs):
    block = pl.BlockSpec((LAYERS, 1, 8 * PACK_HEADS, PADDED), lambda x, h, place: (0, x, h, 0))
    return pl.pallas_call(
        pack_kernel,
        grid_spec=pltpu.PrefetchScalarGridSpec(
            num_scalar_prefetch=1,
            grid=(2, HEADS // PACK_HEADS),
            in_specs=[block, block],
            out_specs=pl.BlockSpec((1, PACK_HEADS, 32, LANES), lambda x, h, place: (x, h, 0, 0)),
        ),
        out_shape=jax.ShapeDtypeStruct((2, HEADS, 32, LANES), jnp.int32),
        name="pack",
    )(place, mine, theirs)


def route_kernel(src_block, group_map, q_slot, words, out, whole_q, where_q):
    r = pl.program_id(0)
    for j in range(GROUP):
        where_q[q_slot[r * GROUP + j]] = j
    lane = lanes_of((8, LANES))
    left = lane < 64
    blocks = [[None] * 10 for _ in range(LAYERS)]
    for pair in range(2):
        even, odd = 2 * pair, 2 * pair + 1
        tiles = {}
        rest = [None] * LAYERS
        for x in range(2):
            third = {}
            for m in (even, odd):
                last = words[x, m, 24:32, :]
                high = high_of(last)
                scales = scale_of(high)
                first = 64 if m == even else 0
                scale = [scales[:, first + l : first + l + 1] for l in range(LAYERS)]
                low = low_of(last).astype(jnp.float32)
                high = high.astype(jnp.float32)
                third[m] = (low * scale[0], low * scale[1], high * scale[2])
                for l in range(LAYERS):
                    word = words[x, m, 8 * l : 8 * l + 8, :]
                    a = low_of(word).astype(jnp.float32) * scale[l]
                    b = high_of(word).astype(jnp.float32) * scale[l]
                    if x == 0:
                        tiles[m, l] = (a, b)
                    else:
                        tiles[m, l] = (tiles[m, l][0] + a, tiles[m, l][1] + b)
            part = [
                jnp.where(left, third[even][0], third[odd][0]),
                jnp.where(left, third[odd][1], third[even][1]),
                jnp.where(left, third[even][2], third[odd][2]),
            ]
            rest = part if x == 0 else [p + q for p, q in zip(rest, part)]
        rest[1] = pltpu.roll(rest[1], 64, 1)
        for l in range(LAYERS):
            blocks[l][5 * pair : 5 * pair + 5] = [
                tiles[even, l][0],
                tiles[even, l][1],
                rest[l],
                tiles[odd, l][0],
                tiles[odd, l][1],
            ]
    codes = []
    for l in range(LAYERS):
        code = codes_of(row_max(*blocks[l]))
        inverse = inverse_scale_of(code)
        codes.append(code)
        for j in range(GROUP):
            whole_q[j, l] = whole(blocks[l][j], inverse)
        key_value = packed(whole(blocks[l][8], inverse), whole(blocks[l][9], inverse))
        for s in range(GROUP_DEVS):
            out[s, 24 + 8 * l : 32 + 8 * l, :] = key_value
    code = jnp.where(lane == 0, codes[0], jnp.where(lane == 1, codes[1], codes[2]))
    for s in range(GROUP_DEVS):
        out[s, 48:56, :] = code
        first, second = where_q[2 * s], where_q[2 * s + 1]
        for l in range(LAYERS):
            out[s, 8 * l : 8 * l + 8, :] = packed(whole_q[first, l], whole_q[second, l])


def route(src_block, group_map, q_slot, words):
    return pl.pallas_call(
        route_kernel,
        grid_spec=pltpu.PrefetchScalarGridSpec(
            num_scalar_prefetch=3,
            grid=(KV_HEADS,),
            in_specs=[
                pl.BlockSpec((2, GROUP_DEVS, 32, LANES), lambda r, src, grp, slot: (0, src[r], 0, 0))
            ],
            out_specs=pl.BlockSpec((GROUP_DEVS, 56, LANES), lambda r, src, grp, slot: (grp[r], 0, 0)),
            scratch_shapes=[
                pltpu.VMEM((GROUP, LAYERS, 8, LANES), jnp.int32),
                pltpu.SMEM((GROUP,), jnp.int32),
            ],
        ),
        out_shape=jax.ShapeDtypeStruct((HEADS, 56, LANES), jnp.int32),
        name="route",
    )(src_block, group_map, q_slot, words)


OPEN_HEADS = 8


def open_kernel(words, out):
    for i in range(OPEN_HEADS):
        scales = scale_of(words[i, 48:56, :])
        rows = slice(8 * i, 8 * i + 8)
        for l in range(LAYERS):
            scale = scales[:, l : l + 1]
            for half in range(2):
                first = 24 * half + 8 * l
                word = words[i, first : first + 8, :]
                cols = 2 * LANES * half
                out[l, rows, cols : cols + LANES] = low_of(word).astype(jnp.float32) * scale
                out[l, rows, cols + LANES : cols + 2 * LANES] = (
                    high_of(word).astype(jnp.float32) * scale
                )


def opened(words):
    return pl.pallas_call(
        open_kernel,
        grid=(HEADS // OPEN_HEADS,),
        in_specs=[pl.BlockSpec((OPEN_HEADS, 56, LANES), lambda h: (h, 0, 0))],
        out_specs=pl.BlockSpec((LAYERS, 8 * OPEN_HEADS, 4 * LANES), lambda h: (0, h, 0)),
        out_shape=jax.ShapeDtypeStruct((LAYERS, SLICE, 4 * LANES), jnp.float32),
        name="opened",
    )(words)


def on_device(hidden, joined_weight, src_block, group_map, q_slot):
    place = jnp.stack([lax.axis_index("core"), lax.axis_index("head") & 1]).astype(jnp.int32)
    weight = jnp.swapaxes(joined_weight, 1, 2)
    away = product(place, hidden, weight, 1)
    theirs = lax.ppermute(away, "core", [(0, 1), (1, 0)])
    mine = product(place, hidden, weight, 0)
    words = pack(place, mine, theirs).reshape(2 * HEADS, 32, LANES)
    words = lax.all_to_all(words, ("near", "head"), 0, 0, tiled=True)
    words = route(src_block, group_map, q_slot, words.reshape(2, HEADS, 32, LANES))
    words = lax.all_to_all(words, "head", 0, 0, tiled=True)
    return opened(words)


def solution(mesh):
    split = Mesh(mesh.devices.reshape(HEADS, 2, 2), ("head", "near", "core"))
    kdim = ("near", "core")
    return jax.shard_map(
        on_device,
        mesh=split,
        in_specs=(P(None, None, kdim), P(None, kdim, "head"), P(), P(), P()),
        out_specs=P(None, kdim, "head"),
        check_vma=False,
    )
```

```python
import jax
import jax.numpy as jnp
from jax import lax
from jax.experimental import pallas as pl
from jax.experimental.pallas import tpu as pltpu
from jax.sharding import Mesh, PartitionSpec as P

LAYERS = 3
ROWS = 1024
SLICE = 256
LANES = 128
WIDTH = 320
PADDED = 384
HEADS = 32
GROUP_DEVS = 4
KV_HEADS = 8
GROUP = 8
CODES = 256.0
TOP = 32700.0


def codes_of(amax):
    return jnp.ceil(CODES * jnp.log2(jnp.maximum(amax, 1e-30) * (1.0 / TOP))).astype(jnp.int32)


def scale_of(code):
    return jnp.exp2(code.astype(jnp.float32) * (1.0 / CODES))


def inverse_scale_of(code):
    return jnp.exp2(code.astype(jnp.float32) * (-1.0 / CODES))


def whole(x, inverse):
    return jnp.round(x * inverse).astype(jnp.int32)


def packed(low, high):
    return (low & 0xFFFF) | (high << 16)


def low_of(words):
    return (words << 16) >> 16


def high_of(words):
    return words >> 16


def row_max(*tiles):
    top = jnp.abs(tiles[0])
    for tile in tiles[1:]:
        top = jnp.maximum(top, jnp.abs(tile))
    return jnp.max(top, axis=1, keepdims=True)


def lanes_of(shape):
    return lax.broadcasted_iota(jnp.int32, shape, 1)


VMEM = pl.BlockSpec(memory_space=pltpu.VMEM)
SMEM = pl.BlockSpec(memory_space=pltpu.SMEM)
HBM = pl.BlockSpec(memory_space=pltpu.HBM)


def limit(mib, **others):
    return pltpu.CompilerParams(vmem_limit_bytes=mib * 1024 * 1024, **others)


def placed(value, odd, out):
    @pl.when(odd == 0)
    def _():
        out[:, :WIDTH] = value
        out[:, WIDTH:] = jnp.zeros((2 * SLICE, PADDED - WIDTH), jnp.float32)

    @pl.when(odd == 1)
    def _():
        out[:, :256] = value[:, 64:]
        out[:, 256:320] = jnp.zeros((2 * SLICE, 64), jnp.float32)
        out[:, 320:] = value[:, :64]


def product_of(rows, weight):
    return lax.dot_general(
        rows, weight, (((1,), (1,)), ((), ())), preferred_element_type=jnp.float32
    )


def away_kernel(place, hidden, weight, out, my_rows, weight_rows, away_rows, arrived):
    core = place[0]

    def rows_copy(l, x, other):
        first = pl.multiple_of((2 * x + (1 - core if other else core)) * SLICE, SLICE)
        target = away_rows if other else my_rows
        return pltpu.make_async_copy(
            hidden.at[l, pl.ds(first, SLICE), :],
            target.at[l, pl.ds(SLICE * x, SLICE), :],
            arrived.at[l, 2 * int(other) + x],
        )

    def weight_copy(l):
        return pltpu.make_async_copy(weight.at[l], weight_rows.at[l], arrived.at[l, 4])

    for l in range(LAYERS):
        weight_copy(l).start()
        for x in range(2):
            rows_copy(l, x, True).start()
    for l in range(LAYERS):
        for x in range(2):
            rows_copy(l, x, False).start()

    @pl.loop(0, LAYERS)
    def _(l):
        weight_copy(l).wait()
        for x in range(2):
            rows_copy(l, x, True).wait()
        placed(product_of(away_rows[l], weight_rows[l]), place[1], out.at[l])

    for l in range(LAYERS):
        for x in range(2):
            rows_copy(l, x, False).wait()


def away_product(place, hidden, weight):
    return pl.pallas_call(
        away_kernel,
        in_specs=[SMEM, HBM, HBM],
        out_specs=[VMEM, VMEM, VMEM],
        scratch_shapes=[
            pltpu.VMEM((LAYERS, 2 * SLICE, 2048), jnp.bfloat16),
            pltpu.SemaphoreType.DMA((LAYERS, 5)),
        ],
        out_shape=[
            pltpu.VMEM((LAYERS, 2 * SLICE, PADDED), jnp.float32),
            pltpu.VMEM((LAYERS, 2 * SLICE, 2048), jnp.bfloat16),
            pltpu.VMEM((LAYERS, WIDTH, 2048), jnp.bfloat16),
        ],
        cost_estimate=pl.CostEstimate(
            flops=LAYERS * 512 * 2048 * WIDTH * 2, bytes_accessed=20_000_000, transcendentals=0
        ),
        compiler_params=limit(44),
        name="away_product",
    )(place, hidden, weight)


def my_kernel(place, rows, weight, out):
    @pl.loop(0, LAYERS)
    def _(l):
        placed(product_of(rows[l], weight[l]), place[1], out.at[l])


def my_product(place, rows, weight):
    return pl.pallas_call(
        my_kernel,
        in_specs=[SMEM, VMEM, VMEM],
        out_specs=VMEM,
        out_shape=jax.ShapeDtypeStruct((LAYERS, 2 * SLICE, PADDED), jnp.float32),
        cost_estimate=pl.CostEstimate(
            flops=LAYERS * 512 * 2048 * WIDTH * 2, bytes_accessed=12_000_000, transcendentals=0
        ),
        compiler_params=limit(24),
        name="my_product",
    )(place, rows, weight)


PACK_HEADS = 8


def pack_kernel(place, mine, theirs, out):
    odd = place[1]
    lane = lanes_of((8, LANES))
    spare = (lane >= 64) != (odd == 1)
    slot = lane & 63
    step = pl.program_id(0)
    for i in range(PACK_HEADS):
        rows = pl.ds(pl.multiple_of(8 * (step * PACK_HEADS + i), 8), 8)
        block = step * PACK_HEADS + i
        rest, codes = [], []
        for l in range(LAYERS):
            tiles = []
            for t in range(3):
                cols = slice(LANES * t, LANES * t + LANES)
                tiles.append(mine[l, rows, cols] + theirs[l, rows, cols])
            code = codes_of(row_max(*tiles))
            inverse = inverse_scale_of(code)
            a, b, c = [whole(tile, inverse) for tile in tiles]
            out[block, 8 * l : 8 * l + 8, :] = packed(a, b)
            rest.append(c)
            codes.append(code)
        code = jnp.where(slot == 0, codes[0], jnp.where(slot == 1, codes[1], codes[2]))
        low = rest[0] + pltpu.roll(rest[1], 64, 1)
        high = jnp.where(spare, code, rest[2])
        out[block, 24:32, :] = packed(low, high)


def pack(place, mine, theirs):
    return pl.pallas_call(
        pack_kernel,
        grid=(2 * HEADS // PACK_HEADS,),
        in_specs=[SMEM, VMEM, VMEM],
        out_specs=VMEM,
        out_shape=jax.ShapeDtypeStruct((2 * HEADS, 32, LANES), jnp.int32),
        compiler_params=limit(16),
        name="pack",
    )(place, mine, theirs)


def route_kernel(src_block, group_map, q_slot, words, out, whole_q, where_q):
    r = pl.program_id(0)
    source = src_block[r] * GROUP_DEVS
    target = group_map[r] * GROUP_DEVS
    for j in range(GROUP):
        where_q[q_slot[r * GROUP + j]] = j
    lane = lanes_of((8, LANES))
    left = lane < 64
    blocks = [[None] * 10 for _ in range(LAYERS)]
    for pair in range(2):
        even, odd = 2 * pair, 2 * pair + 1
        tiles = {}
        rest = [None] * LAYERS
        for x in range(2):
            third = {}
            for m in (even, odd):
                last = words[x * HEADS + source + m, 24:32, :]
                high = high_of(last)
                scales = scale_of(high)
                first = 64 if m == even else 0
                scale = [scales[:, first + l : first + l + 1] for l in range(LAYERS)]
                low = low_of(last).astype(jnp.float32)
                high = high.astype(jnp.float32)
                third[m] = (low * scale[0], low * scale[1], high * scale[2])
                for l in range(LAYERS):
                    word = words[x * HEADS + source + m, 8 * l : 8 * l + 8, :]
                    a = low_of(word).astype(jnp.float32) * scale[l]
                    b = high_of(word).astype(jnp.float32) * scale[l]
                    if x == 0:
                        tiles[m, l] = (a, b)
                    else:
                        tiles[m, l] = (tiles[m, l][0] + a, tiles[m, l][1] + b)
            part = [
                jnp.where(left, third[even][0], third[odd][0]),
                jnp.where(left, third[odd][1], third[even][1]),
                jnp.where(left, third[even][2], third[odd][2]),
            ]
            rest = part if x == 0 else [p + q for p, q in zip(rest, part)]
        rest[1] = pltpu.roll(rest[1], 64, 1)
        for l in range(LAYERS):
            blocks[l][5 * pair : 5 * pair + 5] = [
                tiles[even, l][0],
                tiles[even, l][1],
                rest[l],
                tiles[odd, l][0],
                tiles[odd, l][1],
            ]
    codes = []
    for l in range(LAYERS):
        code = codes_of(row_max(*blocks[l]))
        inverse = inverse_scale_of(code)
        codes.append(code)
        for j in range(GROUP):
            whole_q[j, l] = whole(blocks[l][j], inverse)
        key_value = packed(whole(blocks[l][8], inverse), whole(blocks[l][9], inverse))
        for s in range(GROUP_DEVS):
            out[target + s, 24 + 8 * l : 32 + 8 * l, :] = key_value
    code = jnp.where(lane == 0, codes[0], jnp.where(lane == 1, codes[1], codes[2]))
    for s in range(GROUP_DEVS):
        out[target + s, 48:56, :] = code
        first, second = where_q[2 * s], where_q[2 * s + 1]
        for l in range(LAYERS):
            out[target + s, 8 * l : 8 * l + 8, :] = packed(whole_q[first, l], whole_q[second, l])


def route(src_block, group_map, q_slot, words):
    return pl.pallas_call(
        route_kernel,
        grid=(KV_HEADS,),
        in_specs=[SMEM, SMEM, SMEM, VMEM],
        out_specs=VMEM,
        scratch_shapes=[
            pltpu.VMEM((GROUP, LAYERS, 8, LANES), jnp.int32),
            pltpu.SMEM((GROUP,), jnp.int32),
        ],
        out_shape=jax.ShapeDtypeStruct((HEADS, 56, LANES), jnp.int32),
        compiler_params=limit(16),
        name="route",
    )(src_block, group_map, q_slot, words)


OPEN_HEADS = 8


def open_kernel(words, out):
    for i in range(OPEN_HEADS):
        block = pl.program_id(0) * OPEN_HEADS + i
        scales = scale_of(words[block, 48:56, :])
        rows = slice(8 * i, 8 * i + 8)
        for l in range(LAYERS):
            scale = scales[:, l : l + 1]
            for half in range(2):
                first = 24 * half + 8 * l
                word = words[block, first : first + 8, :]
                cols = 2 * LANES * half
                out[l, rows, cols : cols + LANES] = low_of(word).astype(jnp.float32) * scale
                out[l, rows, cols + LANES : cols + 2 * LANES] = (
                    high_of(word).astype(jnp.float32) * scale
                )


def opened(words):
    return pl.pallas_call(
        open_kernel,
        grid=(HEADS // OPEN_HEADS,),
        in_specs=[VMEM],
        out_specs=pl.BlockSpec((LAYERS, 8 * OPEN_HEADS, 4 * LANES), lambda h: (0, h, 0)),
        out_shape=jax.ShapeDtypeStruct((LAYERS, SLICE, 4 * LANES), jnp.float32),
        compiler_params=limit(16),
        name="opened",
    )(words)


def on_device(hidden, joined_weight, src_block, group_map, q_slot):
    place = jnp.stack([lax.axis_index("core"), lax.axis_index("head") & 1]).astype(jnp.int32)
    hidden = pltpu.with_memory_space_constraint(hidden, pltpu.HBM)
    weight = pltpu.with_memory_space_constraint(jnp.swapaxes(joined_weight, 1, 2), pltpu.HBM)
    away, rows, weight = away_product(place, hidden, weight)
    theirs = lax.ppermute(away, "core", [(0, 1), (1, 0)])
    mine = my_product(place, rows, weight)
    words = pack(place, mine, theirs)
    words = lax.all_to_all(words, ("near", "head"), 0, 0, tiled=True)
    words = route(src_block, group_map, q_slot, words)
    words = lax.all_to_all(words, "head", 0, 0, tiled=True)
    return opened(words)


def solution(mesh):
    split = Mesh(mesh.devices.reshape(HEADS, 2, 2), ("head", "near", "core"))
    kdim = ("near", "core")
    return jax.shard_map(
        on_device,
        mesh=split,
        in_specs=(P(None, None, kdim), P(None, kdim, "head"), P(), P(), P()),
        out_specs=P(None, kdim, "head"),
        check_vma=False,
    )
```

```python
import jax
import jax.numpy as jnp
from jax import lax
from jax.experimental import pallas as pl
from jax.experimental.pallas import tpu as pltpu
from jax.sharding import Mesh, PartitionSpec as P

LAYERS = 3
SLICE = 256
MINE = 2 * SLICE
DEPTH = 2048
LANES = 128
WIDTH = 320
PADDED = 384
HEADS = 32
GROUP_DEVS = 4
KV_HEADS = 8
GROUP = 8
CODES = 256.0
TOP = 32700.0

VMEM = pl.BlockSpec(memory_space=pltpu.VMEM)
SMEM = pl.BlockSpec(memory_space=pltpu.SMEM)
HBM = pl.BlockSpec(memory_space=pltpu.HBM)


def limit(mib):
    return pltpu.CompilerParams(vmem_limit_bytes=mib * 1024 * 1024)


def codes_of(amax):
    return jnp.ceil(CODES * jnp.log2(jnp.maximum(amax, 1e-30) * (1.0 / TOP))).astype(jnp.int32)


def scale_of(code):
    return jnp.exp2(code.astype(jnp.float32) * (1.0 / CODES))


def inverse_scale_of(code):
    return jnp.exp2(code.astype(jnp.float32) * (-1.0 / CODES))


def whole(x):
    return jnp.round(x).astype(jnp.int32)


def packed(low, high):
    return (low & 0xFFFF) | (high << 16)


def low_of(words):
    return (words << 16) >> 16


def high_of(words):
    return words >> 16


def lanes():
    return lax.broadcasted_iota(jnp.int32, (8, LANES), 1)


def product_of(rows, weight):
    return lax.dot_general(
        rows, weight, (((1,), (1,)), ((), ())), preferred_element_type=jnp.float32
    )


def away_kernel(hidden, weight, out, my_rows, weight_rows, away_rows, arrived):
    core = lax.axis_index("core")
    odd = lax.axis_index("head") & 1

    def rows_copy(l, x, other):
        first = pl.multiple_of((2 * x + (1 - core if other else core)) * SLICE, SLICE)
        target = away_rows if other else my_rows
        return pltpu.make_async_copy(
            hidden.at[l, pl.ds(first, SLICE), :],
            target.at[l, pl.ds(SLICE * x, SLICE), :],
            arrived.at[l, 2 * int(other) + x],
        )

    def weight_copies(l):
        blocks = pl.multiple_of(64 * odd, 64)
        half = pl.multiple_of(256 * (1 - odd), 64)
        place = pl.multiple_of(256 + 64 * odd, 64)
        return [
            pltpu.make_async_copy(
                weight.at[l, pl.ds(blocks, 256), :],
                weight_rows.at[l, pl.ds(0, 256), :],
                arrived.at[l, 4],
            ),
            pltpu.make_async_copy(
                weight.at[l, pl.ds(half, 64), :],
                weight_rows.at[l, pl.ds(place, 64), :],
                arrived.at[l, 5],
            ),
        ]

    for l in range(LAYERS):
        for copy in weight_copies(l):
            copy.start()
        for x in range(2):
            rows_copy(l, x, True).start()
    for l in range(LAYERS):
        for x in range(2):
            rows_copy(l, x, False).start()
    nothing = pl.multiple_of(320 - 64 * odd, 64)
    for l in range(LAYERS):
        weight_rows[l, pl.ds(nothing, 64), :] = jnp.zeros((64, DEPTH), jnp.bfloat16)

    @pl.loop(0, LAYERS)
    def _(l):
        for copy in weight_copies(l):
            copy.wait()
        for x in range(2):
            rows_copy(l, x, True).wait()
        out[l] = product_of(away_rows[l], weight_rows[l])

    for l in range(LAYERS):
        for x in range(2):
            rows_copy(l, x, False).wait()


def away_product(hidden, weight):
    return pl.pallas_call(
        away_kernel,
        in_specs=[HBM, HBM],
        out_specs=[VMEM, VMEM, VMEM],
        scratch_shapes=[
            pltpu.VMEM((LAYERS, MINE, DEPTH), jnp.bfloat16),
            pltpu.SemaphoreType.DMA((LAYERS, 6)),
        ],
        out_shape=[
            pltpu.VMEM((LAYERS, MINE, PADDED), jnp.float32),
            pltpu.VMEM((LAYERS, MINE, DEPTH), jnp.bfloat16),
            pltpu.VMEM((LAYERS, PADDED, DEPTH), jnp.bfloat16),
        ],
        cost_estimate=pl.CostEstimate(
            flops=LAYERS * MINE * DEPTH * PADDED * 2, bytes_accessed=20_000_000, transcendentals=0
        ),
        compiler_params=limit(44),
        name="away_product",
    )(hidden, weight)


def my_kernel(rows, weight, out):
    @pl.loop(0, LAYERS)
    def _(l):
        out[l] = product_of(rows[l], weight[l])


def my_product(rows, weight):
    return pl.pallas_call(
        my_kernel,
        in_specs=[VMEM, VMEM],
        out_specs=VMEM,
        out_shape=pltpu.VMEM((LAYERS, MINE, PADDED), jnp.float32),
        cost_estimate=pl.CostEstimate(
            flops=LAYERS * MINE * DEPTH * PADDED * 2, bytes_accessed=12_000_000, transcendentals=0
        ),
        compiler_params=limit(24),
        name="my_product",
    )(rows, weight)


PACK_UNROLL = 8


def pack_kernel(mine, theirs, out):
    lane = lanes()
    odd = lax.axis_index("head") & 1
    spare = (lane >= 64) != (odd == 1)
    slot = lane & 63
    for x in range(2):

        def pack_tiles(step, codes):
            for i in range(PACK_UNROLL):
                head = step * PACK_UNROLL + i
                block = x * HEADS + head
                rows = pl.ds(pl.multiple_of(8 * block, 8), 8)
                tiles = [mine[l, rows, :] + theirs[l, rows, :] for l in range(LAYERS)]
                top = jnp.maximum(
                    jnp.maximum(jnp.abs(tiles[0]), jnp.abs(tiles[1])), jnp.abs(tiles[2])
                )
                code = codes_of(jnp.max(top, axis=1, keepdims=True))
                inverse = inverse_scale_of(code)
                rest = []
                for l in range(LAYERS):
                    a, b, c = [
                        whole(tiles[l][:, LANES * t : LANES * t + LANES] * inverse)
                        for t in range(3)
                    ]
                    out[block, 8 * l : 8 * l + 8, :] = packed(a, b)
                    rest.append(c)
                low = rest[0] + pltpu.roll(rest[1], 64, 1)
                out[block, 24:32, :] = packed(low, jnp.where(spare, code, rest[2]))
                codes = jnp.where(slot == head, code, codes)
            return codes

        codes = lax.fori_loop(
            0, HEADS // PACK_UNROLL, pack_tiles, jnp.zeros((8, LANES), jnp.int32)
        )
        codes = codes << 16
        shown = spare & (slot < HEADS)

        @pl.loop(0, HEADS // PACK_UNROLL)
        def _(step):
            for i in range(PACK_UNROLL):
                block = x * HEADS + step * PACK_UNROLL + i
                word = out[block, 24:32, :]
                out[block, 24:32, :] = jnp.where(shown, (word & 0xFFFF) | codes, word)


def pack(mine, theirs):
    return pl.pallas_call(
        pack_kernel,
        in_specs=[VMEM, VMEM],
        out_specs=VMEM,
        out_shape=pltpu.VMEM((2 * HEADS, 32, LANES), jnp.int32),
        compiler_params=limit(16),
        name="pack",
    )(mine, theirs)


def route_kernel(table, words, out, scales, whole_q, where_q):
    reach = []
    for x in range(2):
        tops = []
        for parity in range(2):
            top = None
            for m in range(parity, HEADS, 2):
                code = high_of(words[x * HEADS + m, 24:32, :])
                top = code if top is None else jnp.maximum(top, code)
            tops.append(top)
        reach.append(scale_of(jnp.maximum(tops[0], pltpu.roll(tops[1], 64, 1))))
    reach = reach[0] + reach[1]
    scales[...] = reach
    inverse = 1.0 / reach[:, 96:97]
    left = lanes() < 64

    @pl.loop(0, KV_HEADS)
    def _(r):
        source = table[r] * GROUP_DEVS
        target = table[KV_HEADS + r] * GROUP_DEVS
        for j in range(GROUP):
            where_q[table[2 * KV_HEADS + r * GROUP + j]] = j
        blocks = [[None] * 10 for _ in range(LAYERS)]
        for pair in range(2):
            even, odd = 2 * pair, 2 * pair + 1
            tiles = {}
            rest = None
            for x in range(2):
                third = {}
                for m in (even, odd):
                    device = x * HEADS + source + m
                    last = words[device, 24:32, :]
                    low, high = low_of(last), high_of(last)
                    at = 96 if m == even else 32
                    ratio = scale_of(high[:, at : at + 1]) * inverse
                    third[m] = (low.astype(jnp.float32) * ratio, high.astype(jnp.float32) * ratio)
                    for l in range(LAYERS):
                        word = words[device, 8 * l : 8 * l + 8, :]
                        a = low_of(word).astype(jnp.float32) * ratio
                        b = high_of(word).astype(jnp.float32) * ratio
                        if x == 0:
                            tiles[m, l] = (a, b)
                        else:
                            tiles[m, l] = (tiles[m, l][0] + a, tiles[m, l][1] + b)
                part = [
                    jnp.where(left, third[even][0], third[odd][0]),
                    jnp.where(left, third[odd][0], third[even][0]),
                    jnp.where(left, third[even][1], third[odd][1]),
                ]
                rest = part if x == 0 else [p + q for p, q in zip(rest, part)]
            rest[1] = pltpu.roll(rest[1], 64, 1)
            for l in range(LAYERS):
                blocks[l][5 * pair : 5 * pair + 5] = [
                    tiles[even, l][0],
                    tiles[even, l][1],
                    rest[l],
                    tiles[odd, l][0],
                    tiles[odd, l][1],
                ]
        for l in range(LAYERS):
            for j in range(GROUP):
                whole_q[j, l] = whole(blocks[l][j])
            key_value = packed(whole(blocks[l][8]), whole(blocks[l][9]))
            for s in range(GROUP_DEVS):
                out[target + s, 24 + 8 * l : 32 + 8 * l, :] = key_value
        for s in range(GROUP_DEVS):
            first, second = where_q[2 * s] & 7, where_q[2 * s + 1] & 7
            for l in range(LAYERS):
                out[target + s, 8 * l : 8 * l + 8, :] = packed(whole_q[first, l], whole_q[second, l])


def route(table, words):
    return pl.pallas_call(
        route_kernel,
        in_specs=[SMEM, VMEM],
        out_specs=[VMEM, VMEM],
        scratch_shapes=[
            pltpu.VMEM((GROUP, LAYERS, 8, LANES), jnp.int32),
            pltpu.SMEM((GROUP,), jnp.int32),
        ],
        out_shape=[
            pltpu.VMEM((HEADS, 48, LANES), jnp.int32),
            pltpu.VMEM((8, LANES), jnp.float32),
        ],
        compiler_params=limit(16),
        name="route",
    )(table, words)


OPEN_HEADS = 8


def open_kernel(words, scales, out):
    step = pl.program_id(0)
    scale_columns = pltpu.roll(scales[...], 64 - OPEN_HEADS * step, 1)
    for i in range(OPEN_HEADS):
        block = step * OPEN_HEADS + i
        scale = scale_columns[:, i : i + 1]
        rows = slice(8 * i, 8 * i + 8)
        for l in range(LAYERS):
            for half in range(2):
                first = 24 * half + 8 * l
                word = words[block, first : first + 8, :]
                cols = 2 * LANES * half
                out[l, rows, cols : cols + LANES] = low_of(word).astype(jnp.float32) * scale
                out[l, rows, cols + LANES : cols + 2 * LANES] = (
                    high_of(word).astype(jnp.float32) * scale
                )


def opened(words, scales):
    return pl.pallas_call(
        open_kernel,
        grid=(HEADS // OPEN_HEADS,),
        in_specs=[VMEM, VMEM],
        out_specs=pl.BlockSpec((LAYERS, 8 * OPEN_HEADS, 4 * LANES), lambda h: (0, h, 0)),
        out_shape=jax.ShapeDtypeStruct((LAYERS, SLICE, 4 * LANES), jnp.float32),
        compiler_params=limit(16),
        name="opened",
    )(words, scales)


def on_device(hidden, joined_weight, src_block, group_map, q_slot):
    hidden = pltpu.with_memory_space_constraint(hidden, pltpu.HBM)
    weight = pltpu.with_memory_space_constraint(jnp.swapaxes(joined_weight, 1, 2), pltpu.HBM)
    away, rows, weight = away_product(hidden, weight)
    theirs = lax.ppermute(away, "core", [(0, 1), (1, 0)])
    mine = my_product(rows, weight)
    table = jnp.concatenate([src_block, group_map, q_slot])
    mine, table = lax.optimization_barrier((mine, table))
    words = pack(mine, theirs)
    words = lax.all_to_all(words, ("near", "head"), 0, 0, tiled=True)
    words, scales = route(table, words)
    words = lax.all_to_all(words, "head", 0, 0, tiled=True)
    return opened(words, scales)


def solution(mesh):
    split = Mesh(mesh.devices.reshape(HEADS, 2, 2), ("head", "near", "core"))
    kdim = ("near", "core")
    return jax.shard_map(
        on_device,
        mesh=split,
        in_specs=(P(None, None, kdim), P(None, kdim, "head"), P(), P(), P()),
        out_specs=P(None, kdim, "head"),
        check_vma=False,
    )
```

```python
import jax
import jax.numpy as jnp
from jax import lax
from jax.experimental import pallas as pl
from jax.experimental.pallas import tpu as pltpu
from jax.sharding import Mesh, PartitionSpec as P

LAYERS = 3
SLICE = 256
MINE = 2 * SLICE
DEPTH = 2048
LANES = 128
WIDTH = 320
PADDED = 384
EARLY = 2
HEADS = 32
GROUP_DEVS = 4
KV_HEADS = 8
GROUP = 8
CODES = 256.0
TOP = 32700.0

VMEM = pl.BlockSpec(memory_space=pltpu.VMEM)
SMEM = pl.BlockSpec(memory_space=pltpu.SMEM)
HBM = pl.BlockSpec(memory_space=pltpu.HBM)


def limit(mib):
    return pltpu.CompilerParams(vmem_limit_bytes=mib * 1024 * 1024)


def codes_of(amax):
    return jnp.ceil(CODES * jnp.log2(jnp.maximum(amax, 1e-30) * (1.0 / TOP))).astype(jnp.int32)


def scale_of(code):
    return jnp.exp2(code.astype(jnp.float32) * (1.0 / CODES))


def inverse_scale_of(code):
    return jnp.exp2(code.astype(jnp.float32) * (-1.0 / CODES))


def whole(x):
    return jnp.round(x).astype(jnp.int32)


def packed(low, high):
    return (low & 0xFFFF) | (high << 16)


def low_of(words):
    return (words << 16) >> 16


def high_of(words):
    return words >> 16


def lanes():
    return lax.broadcasted_iota(jnp.int32, (8, LANES), 1)


def product_of(rows, weight):
    return lax.dot_general(
        rows, weight, (((1,), (1,)), ((), ())), preferred_element_type=jnp.float32
    )


def away_kernel(hidden, weight, out, my_rows, weight_rows, away_rows, arrived):
    core = lax.axis_index("core")
    odd = lax.axis_index("head") & 1

    def rows_copy(l, x, other):
        first = pl.multiple_of((2 * x + (1 - core if other else core)) * SLICE, SLICE)
        target = away_rows if other else my_rows
        return pltpu.make_async_copy(
            hidden.at[l, pl.ds(first, SLICE), :],
            target.at[l, pl.ds(SLICE * x, SLICE), :],
            arrived.at[l, 2 * int(other) + x],
        )

    def weight_copies(l):
        blocks = pl.multiple_of(64 * odd, 64)
        half = pl.multiple_of(256 * (1 - odd), 64)
        place = pl.multiple_of(256 + 64 * odd, 64)
        return [
            pltpu.make_async_copy(
                weight.at[l, pl.ds(blocks, 256), :],
                weight_rows.at[l, pl.ds(0, 256), :],
                arrived.at[l, 4],
            ),
            pltpu.make_async_copy(
                weight.at[l, pl.ds(half, 64), :],
                weight_rows.at[l, pl.ds(place, 64), :],
                arrived.at[l, 5],
            ),
        ]

    for l in range(LAYERS):
        for copy in weight_copies(l):
            copy.start()
        for x in range(2):
            rows_copy(l, x, True).start()
    for l in range(EARLY):
        for x in range(2):
            rows_copy(l, x, False).start()
    nothing = pl.multiple_of(320 - 64 * odd, 64)
    for l in range(LAYERS):
        weight_rows[l, pl.ds(nothing, 64), :] = jnp.zeros((64, DEPTH), jnp.bfloat16)

    @pl.loop(0, LAYERS)
    def _(l):
        for copy in weight_copies(l):
            copy.wait()
        for x in range(2):
            rows_copy(l, x, True).wait()
        out[l] = product_of(away_rows[l], weight_rows[l])

    for l in range(EARLY):
        for x in range(2):
            rows_copy(l, x, False).wait()


def away_product(hidden, weight):
    return pl.pallas_call(
        away_kernel,
        in_specs=[HBM, HBM],
        out_specs=[VMEM, VMEM, VMEM],
        scratch_shapes=[
            pltpu.VMEM((LAYERS, MINE, DEPTH), jnp.bfloat16),
            pltpu.SemaphoreType.DMA((LAYERS, 6)),
        ],
        out_shape=[
            pltpu.VMEM((LAYERS, MINE, PADDED), jnp.float32),
            pltpu.VMEM((EARLY, MINE, DEPTH), jnp.bfloat16),
            pltpu.VMEM((LAYERS, PADDED, DEPTH), jnp.bfloat16),
        ],
        cost_estimate=pl.CostEstimate(
            flops=LAYERS * MINE * DEPTH * PADDED * 2, bytes_accessed=20_000_000, transcendentals=0
        ),
        compiler_params=limit(44),
        name="away_product",
    )(hidden, weight)


def my_kernel(
    hidden, rows, weight, src, grp, slot, out, src_out, grp_out, slot_out, late, arrived
):
    core = lax.axis_index("core")
    copies = []
    for x in range(2):
        first = pl.multiple_of((2 * x + core) * SLICE, SLICE)
        copies.append(
            pltpu.make_async_copy(
                hidden.at[EARLY, pl.ds(first, SLICE), :],
                late.at[pl.ds(SLICE * x, SLICE), :],
                arrived.at[x],
            )
        )
    for k, (here, there) in enumerate(((src, src_out), (grp, grp_out), (slot, slot_out))):
        copies.append(pltpu.make_async_copy(here, there, arrived.at[2 + k]))
    for copy in copies:
        copy.start()

    for l in range(EARLY):
        out[l] = product_of(rows[l], weight[l])
    for copy in copies:
        copy.wait()
    out[EARLY] = product_of(late[...], weight[EARLY])


def my_product(hidden, rows, weight, src_block, group_map, q_slot):
    return pl.pallas_call(
        my_kernel,
        in_specs=[HBM, VMEM, VMEM, HBM, HBM, HBM],
        out_specs=[VMEM, SMEM, SMEM, SMEM],
        scratch_shapes=[
            pltpu.VMEM((MINE, DEPTH), jnp.bfloat16),
            pltpu.SemaphoreType.DMA((5,)),
        ],
        out_shape=[
            pltpu.VMEM((LAYERS, MINE, PADDED), jnp.float32),
            pltpu.SMEM((KV_HEADS,), jnp.int32),
            pltpu.SMEM((KV_HEADS,), jnp.int32),
            pltpu.SMEM((KV_HEADS * GROUP,), jnp.int32),
        ],
        cost_estimate=pl.CostEstimate(
            flops=LAYERS * MINE * DEPTH * PADDED * 2, bytes_accessed=12_000_000, transcendentals=0
        ),
        compiler_params=limit(24),
        name="my_product",
    )(hidden, rows, weight, src_block, group_map, q_slot)


PACK_UNROLL = 16


def pack_kernel(mine, theirs, out):
    lane = lanes()
    odd = lax.axis_index("head") & 1
    spare = (lane >= 64) != (odd == 1)
    slot = lane & 63
    for x in range(2):

        def pack_tiles(step, codes):
            for i in range(PACK_UNROLL):
                head = step * PACK_UNROLL + i
                block = x * HEADS + head
                rows = pl.ds(pl.multiple_of(8 * block, 8), 8)
                tiles = [mine[l, rows, :] + theirs[l, rows, :] for l in range(LAYERS)]
                top = jnp.maximum(
                    jnp.maximum(jnp.abs(tiles[0]), jnp.abs(tiles[1])), jnp.abs(tiles[2])
                )
                code = codes_of(jnp.max(top, axis=1, keepdims=True))
                inverse = inverse_scale_of(code)
                rest = []
                for l in range(LAYERS):
                    a, b, c = [
                        whole(tiles[l][:, LANES * t : LANES * t + LANES] * inverse)
                        for t in range(3)
                    ]
                    out[block, 8 * l : 8 * l + 8, :] = packed(a, b)
                    rest.append(c)
                low = rest[0] + pltpu.roll(rest[1], 64, 1)
                out[block, 24:32, :] = packed(low, jnp.where(spare, code, rest[2]))
                codes = jnp.where(slot == head, code, codes)
            return codes

        codes = lax.fori_loop(
            0, HEADS // PACK_UNROLL, pack_tiles, jnp.zeros((8, LANES), jnp.int32)
        )
        codes = codes << 16
        shown = spare & (slot < HEADS)

        @pl.loop(0, HEADS // PACK_UNROLL)
        def _(step):
            for i in range(PACK_UNROLL):
                block = x * HEADS + step * PACK_UNROLL + i
                word = out[block, 24:32, :]
                out[block, 24:32, :] = jnp.where(shown, (word & 0xFFFF) | codes, word)


def pack(mine, theirs):
    return pl.pallas_call(
        pack_kernel,
        in_specs=[VMEM, VMEM],
        out_specs=VMEM,
        out_shape=pltpu.VMEM((2 * HEADS, 32, LANES), jnp.int32),
        compiler_params=limit(16),
        name="pack",
    )(mine, theirs)


def route_kernel(src, grp, slot, words, out, scales, whole_q, where_q):
    reach = []
    for x in range(2):
        tops = []
        for parity in range(2):
            top = None
            for m in range(parity, HEADS, 2):
                code = high_of(words[x * HEADS + m, 24:32, :])
                top = code if top is None else jnp.maximum(top, code)
            tops.append(top)
        reach.append(scale_of(jnp.maximum(tops[0], pltpu.roll(tops[1], 64, 1))))
    reach = reach[0] + reach[1]
    scales[...] = reach
    inverse = 1.0 / reach[:, 96:97]
    left = lanes() < 64

    @pl.loop(0, KV_HEADS, unroll=True)
    def _(r):
        source = src[r] * GROUP_DEVS
        target = grp[r] * GROUP_DEVS
        for j in range(GROUP):
            where_q[slot[r * GROUP + j]] = j
        blocks = [[None] * 10 for _ in range(LAYERS)]
        for pair in range(2):
            even, odd = 2 * pair, 2 * pair + 1
            tiles = {}
            rest = None
            for x in range(2):
                third = {}
                for m in (even, odd):
                    device = x * HEADS + source + m
                    last = words[device, 24:32, :]
                    low, high = low_of(last), high_of(last)
                    at = 96 if m == even else 32
                    ratio = scale_of(high[:, at : at + 1]) * inverse
                    third[m] = (low.astype(jnp.float32) * ratio, high.astype(jnp.float32) * ratio)
                    for l in range(LAYERS):
                        word = words[device, 8 * l : 8 * l + 8, :]
                        a = low_of(word).astype(jnp.float32) * ratio
                        b = high_of(word).astype(jnp.float32) * ratio
                        if x == 0:
                            tiles[m, l] = (a, b)
                        else:
                            tiles[m, l] = (tiles[m, l][0] + a, tiles[m, l][1] + b)
                part = [
                    jnp.where(left, third[even][0], third[odd][0]),
                    jnp.where(left, third[odd][0], third[even][0]),
                    jnp.where(left, third[even][1], third[odd][1]),
                ]
                rest = part if x == 0 else [p + q for p, q in zip(rest, part)]
            rest[1] = pltpu.roll(rest[1], 64, 1)
            for l in range(LAYERS):
                blocks[l][5 * pair : 5 * pair + 5] = [
                    tiles[even, l][0],
                    tiles[even, l][1],
                    rest[l],
                    tiles[odd, l][0],
                    tiles[odd, l][1],
                ]
        for l in range(LAYERS):
            for j in range(GROUP):
                whole_q[j, l] = whole(blocks[l][j])
            key_value = packed(whole(blocks[l][8]), whole(blocks[l][9]))
            for s in range(GROUP_DEVS):
                out[target + s, 24 + 8 * l : 32 + 8 * l, :] = key_value
        for s in range(GROUP_DEVS):
            first, second = where_q[2 * s] & 7, where_q[2 * s + 1] & 7
            for l in range(LAYERS):
                out[target + s, 8 * l : 8 * l + 8, :] = packed(whole_q[first, l], whole_q[second, l])


def route(src, grp, slot, words):
    return pl.pallas_call(
        route_kernel,
        in_specs=[SMEM, SMEM, SMEM, VMEM],
        out_specs=[VMEM, VMEM],
        scratch_shapes=[
            pltpu.VMEM((GROUP, LAYERS, 8, LANES), jnp.int32),
            pltpu.SMEM((GROUP,), jnp.int32),
        ],
        out_shape=[
            pltpu.VMEM((HEADS, 48, LANES), jnp.int32),
            pltpu.VMEM((8, LANES), jnp.float32),
        ],
        compiler_params=limit(16),
        name="route",
    )(src, grp, slot, words)


OPEN_HEADS = 16


def open_kernel(words, scales, out):
    step = pl.program_id(0)
    scale_columns = pltpu.roll(scales[...], 64 - OPEN_HEADS * step, 1)
    for i in range(OPEN_HEADS):
        block = step * OPEN_HEADS + i
        scale = scale_columns[:, i : i + 1]
        rows = slice(8 * i, 8 * i + 8)
        for l in range(LAYERS):
            for half in range(2):
                first = 24 * half + 8 * l
                word = words[block, first : first + 8, :]
                cols = 2 * LANES * half
                out[l, rows, cols : cols + LANES] = low_of(word).astype(jnp.float32) * scale
                out[l, rows, cols + LANES : cols + 2 * LANES] = (
                    high_of(word).astype(jnp.float32) * scale
                )


def opened(words, scales):
    return pl.pallas_call(
        open_kernel,
        grid=(HEADS // OPEN_HEADS,),
        in_specs=[VMEM, VMEM],
        out_specs=pl.BlockSpec((LAYERS, 8 * OPEN_HEADS, 4 * LANES), lambda h: (0, h, 0)),
        out_shape=jax.ShapeDtypeStruct((LAYERS, SLICE, 4 * LANES), jnp.float32),
        compiler_params=limit(16),
        name="opened",
    )(words, scales)


def on_device(hidden, joined_weight, src_block, group_map, q_slot):
    hidden = pltpu.with_memory_space_constraint(hidden, pltpu.HBM)
    weight = pltpu.with_memory_space_constraint(jnp.swapaxes(joined_weight, 1, 2), pltpu.HBM)
    away, rows, weight = away_product(hidden, weight)
    theirs = lax.ppermute(away, "core", [(0, 1), (1, 0)])
    tables = [pltpu.with_memory_space_constraint(t, pltpu.HBM) for t in (src_block, group_map, q_slot)]
    mine, *tables = my_product(hidden, rows, weight, *tables)
    words = pack(mine, theirs)
    words = lax.all_to_all(words, ("near", "head"), 0, 0, tiled=True)
    words, scales = route(*tables, words)
    words = lax.all_to_all(words, "head", 0, 0, tiled=True)
    return opened(words, scales)


def solution(mesh):
    split = Mesh(mesh.devices.reshape(HEADS, 2, 2), ("head", "near", "core"))
    kdim = ("near", "core")
    return jax.shard_map(
        on_device,
        mesh=split,
        in_specs=(P(None, None, kdim), P(None, kdim, "head"), P(), P(), P()),
        out_specs=P(None, kdim, "head"),
        check_vma=False,
    )
```

```python
import jax
import jax.numpy as jnp
from jax import lax
from jax.experimental import pallas as pl
from jax.experimental.pallas import tpu as pltpu
from jax.sharding import Mesh, PartitionSpec as P

LAYERS = 3
SLICE = 256
MINE = 2 * SLICE
DEPTH = 2048
LANES = 128
WIDTH = 320
EARLY = 2
HEADS = 32
GROUP_DEVS = 4
KV_HEADS = 8
GROUP = 8
CODES = 256.0
TOP = 32700.0

VMEM = pl.BlockSpec(memory_space=pltpu.VMEM)
SMEM = pl.BlockSpec(memory_space=pltpu.SMEM)
HBM = pl.BlockSpec(memory_space=pltpu.HBM)


def limit(mib):
    return pltpu.CompilerParams(vmem_limit_bytes=mib * 1024 * 1024)


def codes_of(amax):
    return jnp.ceil(CODES * jnp.log2(jnp.maximum(amax, 1e-30) * (1.0 / TOP))).astype(jnp.int32)


def scale_of(code):
    return jnp.exp2(code.astype(jnp.float32) * (1.0 / CODES))


def inverse_scale_of(code):
    return jnp.exp2(code.astype(jnp.float32) * (-1.0 / CODES))


def whole(x):
    return jnp.round(x).astype(jnp.int32)


def packed(low, high):
    return (low & 0xFFFF) | (high << 16)


def low_of(words):
    return (words << 16) >> 16


def high_of(words):
    return words >> 16


def lanes():
    return lax.broadcasted_iota(jnp.int32, (8, LANES), 1)


def product_of(rows, weight):
    return lax.dot_general(
        weight, rows, (((1,), (1,)), ((), ())), preferred_element_type=jnp.float32
    )


def away_kernel(hidden, weight, out, my_rows, weight_rows, away_rows, arrived):
    core = lax.axis_index("core")
    odd = lax.axis_index("head") & 1

    def rows_copy(l, x, other):
        first = pl.multiple_of((2 * x + (1 - core if other else core)) * SLICE, SLICE)
        target = away_rows if other else my_rows
        return pltpu.make_async_copy(
            hidden.at[l, pl.ds(first, SLICE), :],
            target.at[l, pl.ds(SLICE * x, SLICE), :],
            arrived.at[l, 2 * int(other) + x],
        )

    def weight_copies(l):
        blocks = pl.multiple_of(64 * odd, 64)
        half = pl.multiple_of(256 * (1 - odd), 64)
        return [
            pltpu.make_async_copy(
                weight.at[l, pl.ds(blocks, 256), :],
                weight_rows.at[l, pl.ds(0, 256), :],
                arrived.at[l, 4],
            ),
            pltpu.make_async_copy(
                weight.at[l, pl.ds(half, 64), :],
                weight_rows.at[l, pl.ds(256, 64), :],
                arrived.at[l, 5],
            ),
        ]

    for l in range(LAYERS):
        for copy in weight_copies(l):
            copy.start()
        for x in range(2):
            rows_copy(l, x, True).start()
    for l in range(EARLY):
        for x in range(2):
            rows_copy(l, x, False).start()

    @pl.loop(0, LAYERS)
    def _(l):
        for copy in weight_copies(l):
            copy.wait()
        for x in range(2):
            rows_copy(l, x, True).wait()
        out[l] = product_of(away_rows[l], weight_rows[l])

    for l in range(EARLY):
        for x in range(2):
            rows_copy(l, x, False).wait()


def away_product(hidden, weight):
    return pl.pallas_call(
        away_kernel,
        in_specs=[HBM, HBM],
        out_specs=[VMEM, VMEM, VMEM],
        scratch_shapes=[
            pltpu.VMEM((LAYERS, MINE, DEPTH), jnp.bfloat16),
            pltpu.SemaphoreType.DMA((LAYERS, 6)),
        ],
        out_shape=[
            pltpu.VMEM((LAYERS, WIDTH, MINE), jnp.float32),
            pltpu.VMEM((EARLY, MINE, DEPTH), jnp.bfloat16),
            pltpu.VMEM((LAYERS, WIDTH, DEPTH), jnp.bfloat16),
        ],
        cost_estimate=pl.CostEstimate(
            flops=LAYERS * MINE * DEPTH * WIDTH * 2, bytes_accessed=20_000_000, transcendentals=0
        ),
        compiler_params=limit(44),
        name="away_product",
    )(hidden, weight)


def my_kernel(
    hidden, rows, weight, src, grp, slot, out, src_out, grp_out, slot_out, late, arrived
):
    core = lax.axis_index("core")
    copies = []
    for x in range(2):
        first = pl.multiple_of((2 * x + core) * SLICE, SLICE)
        copies.append(
            pltpu.make_async_copy(
                hidden.at[EARLY, pl.ds(first, SLICE), :],
                late.at[pl.ds(SLICE * x, SLICE), :],
                arrived.at[x],
            )
        )
    for k, (here, there) in enumerate(((src, src_out), (grp, grp_out), (slot, slot_out))):
        copies.append(pltpu.make_async_copy(here, there, arrived.at[2 + k]))
    for copy in copies:
        copy.start()

    @pl.loop(0, EARLY)
    def _(l):
        out[l] = product_of(rows[l], weight[l])

    for copy in copies:
        copy.wait()
    out[EARLY] = product_of(late[...], weight[EARLY])


def my_product(hidden, rows, weight, src_block, group_map, q_slot):
    return pl.pallas_call(
        my_kernel,
        in_specs=[HBM, VMEM, VMEM, HBM, HBM, HBM],
        out_specs=[VMEM, SMEM, SMEM, SMEM],
        scratch_shapes=[
            pltpu.VMEM((MINE, DEPTH), jnp.bfloat16),
            pltpu.SemaphoreType.DMA((5,)),
        ],
        out_shape=[
            pltpu.VMEM((LAYERS, WIDTH, MINE), jnp.float32),
            pltpu.SMEM((KV_HEADS,), jnp.int32),
            pltpu.SMEM((KV_HEADS,), jnp.int32),
            pltpu.SMEM((KV_HEADS * GROUP,), jnp.int32),
        ],
        cost_estimate=pl.CostEstimate(
            flops=LAYERS * MINE * DEPTH * WIDTH * 2, bytes_accessed=12_000_000, transcendentals=0
        ),
        compiler_params=limit(24),
        name="my_product",
    )(hidden, rows, weight, src_block, group_map, q_slot)


TILES = LANES // 8


def pack_kernel(mine, theirs, out):
    lane = lanes()
    odd = lax.axis_index("head") & 1
    is_odd = odd == 1
    spare = (lane >= 64) != is_odd
    slot = lane & 63

    @pl.loop(0, 2)
    def _(x):
        codes = jnp.zeros((8, LANES), jnp.int32)
        for j in range(SLICE // LANES):
            tokens = pl.ds(pl.multiple_of(x * SLICE + j * LANES, LANES), LANES)

            def sums(l, first, size):
                rows = pl.ds(first, size)
                return mine[l, rows, tokens] + theirs[l, rows, tokens]

            top = None
            for l in range(LAYERS):
                for first in range(0, WIDTH, 8):
                    value = jnp.abs(sums(l, first, 8))
                    top = value if top is None else jnp.maximum(top, value)
            code = codes_of(jnp.max(top, axis=0, keepdims=True))
            inverse = inverse_scale_of(code)
            first_tile = x * HEADS + j * TILES
            rest = []
            for l in range(LAYERS):
                a = whole(sums(l, 0, LANES) * inverse)
                b = whole(sums(l, LANES, LANES) * inverse)
                words = packed(a, b).T.reshape(TILES, 8, LANES)
                out[pl.ds(first_tile, TILES), 8 * l : 8 * l + 8, :] = words
                rest.append(whole(sums(l, 2 * LANES, 64) * inverse))
            shown = jnp.broadcast_to(code, (64, LANES))
            low = jnp.concatenate(
                [jnp.where(is_odd, rest[1], rest[0]), jnp.where(is_odd, rest[0], rest[1])], axis=0
            )
            high = jnp.concatenate(
                [jnp.where(is_odd, shown, rest[2]), jnp.where(is_odd, rest[2], shown)], axis=0
            )
            words = packed(low, high).T.reshape(TILES, 8, LANES)
            out[pl.ds(first_tile, TILES), 24:32, :] = words
            for i in range(TILES):
                codes = jnp.where(slot == j * TILES + i, words[i], codes)
        codes = codes & ~0xFFFF
        shown = spare & (slot < HEADS)
        for i in range(HEADS):
            word = out[x * HEADS + i, 24:32, :]
            out[x * HEADS + i, 24:32, :] = jnp.where(shown, (word & 0xFFFF) | codes, word)


def pack(mine, theirs):
    return pl.pallas_call(
        pack_kernel,
        in_specs=[VMEM, VMEM],
        out_specs=VMEM,
        out_shape=pltpu.VMEM((2 * HEADS, 32, LANES), jnp.int32),
        compiler_params=limit(16),
        name="pack",
    )(mine, theirs)


def route_kernel(src, grp, slot, words, out, scales, whole_q, where_q):
    reach = []
    for x in range(2):
        tops = []
        for parity in range(2):
            top = None
            for m in range(parity, HEADS, 2):
                code = high_of(words[x * HEADS + m, 24:32, :])
                top = code if top is None else jnp.maximum(top, code)
            tops.append(top)
        reach.append(scale_of(jnp.maximum(tops[0], pltpu.roll(tops[1], 64, 1))))
    reach = reach[0] + reach[1]
    scales[...] = reach
    inverse = 1.0 / reach[:, 96:97]
    left = lanes() < 64

    @pl.loop(0, KV_HEADS, unroll=True)
    def _(r):
        source = src[r] * GROUP_DEVS
        target = grp[r] * GROUP_DEVS
        for j in range(GROUP):
            where_q[slot[r * GROUP + j]] = j
        blocks = [[None] * 10 for _ in range(LAYERS)]
        for pair in range(2):
            even, odd = 2 * pair, 2 * pair + 1
            tiles = {}
            rest = None
            for x in range(2):
                third = {}
                for m in (even, odd):
                    device = x * HEADS + source + m
                    last = words[device, 24:32, :]
                    low, high = low_of(last), high_of(last)
                    at = 96 if m == even else 32
                    ratio = scale_of(high[:, at : at + 1]) * inverse
                    third[m] = (low.astype(jnp.float32) * ratio, high.astype(jnp.float32) * ratio)
                    for l in range(LAYERS):
                        word = words[device, 8 * l : 8 * l + 8, :]
                        a = low_of(word).astype(jnp.float32) * ratio
                        b = high_of(word).astype(jnp.float32) * ratio
                        if x == 0:
                            tiles[m, l] = (a, b)
                        else:
                            tiles[m, l] = (tiles[m, l][0] + a, tiles[m, l][1] + b)
                part = [
                    jnp.where(left, third[even][0], third[odd][0]),
                    jnp.where(left, third[odd][0], third[even][0]),
                    jnp.where(left, third[even][1], third[odd][1]),
                ]
                rest = part if x == 0 else [p + q for p, q in zip(rest, part)]
            rest[1] = pltpu.roll(rest[1], 64, 1)
            for l in range(LAYERS):
                blocks[l][5 * pair : 5 * pair + 5] = [
                    tiles[even, l][0],
                    tiles[even, l][1],
                    rest[l],
                    tiles[odd, l][0],
                    tiles[odd, l][1],
                ]
        for l in range(LAYERS):
            for j in range(GROUP):
                whole_q[j, l] = whole(blocks[l][j])
            key_value = packed(whole(blocks[l][8]), whole(blocks[l][9]))
            for s in range(GROUP_DEVS):
                out[target + s, 24 + 8 * l : 32 + 8 * l, :] = key_value
        for s in range(GROUP_DEVS):
            first, second = where_q[2 * s] & 7, where_q[2 * s + 1] & 7
            for l in range(LAYERS):
                out[target + s, 8 * l : 8 * l + 8, :] = packed(whole_q[first, l], whole_q[second, l])


def route(src, grp, slot, words):
    return pl.pallas_call(
        route_kernel,
        in_specs=[SMEM, SMEM, SMEM, VMEM],
        out_specs=[VMEM, VMEM],
        scratch_shapes=[
            pltpu.VMEM((GROUP, LAYERS, 8, LANES), jnp.int32),
            pltpu.SMEM((GROUP,), jnp.int32),
        ],
        out_shape=[
            pltpu.VMEM((HEADS, 48, LANES), jnp.int32),
            pltpu.VMEM((8, LANES), jnp.float32),
        ],
        compiler_params=limit(16),
        name="route",
    )(src, grp, slot, words)


OPEN_HEADS = 16


def open_kernel(words, scales, out):
    step = pl.program_id(0)
    scale_columns = pltpu.roll(scales[...], 64 - OPEN_HEADS * step, 1)
    for i in range(OPEN_HEADS):
        block = step * OPEN_HEADS + i
        scale = scale_columns[:, i : i + 1]
        rows = slice(8 * i, 8 * i + 8)
        for l in range(LAYERS):
            for half in range(2):
                first = 24 * half + 8 * l
                word = words[block, first : first + 8, :]
                cols = 2 * LANES * half
                out[l, rows, cols : cols + LANES] = low_of(word).astype(jnp.float32) * scale
                out[l, rows, cols + LANES : cols + 2 * LANES] = (
                    high_of(word).astype(jnp.float32) * scale
                )


def opened(words, scales):
    return pl.pallas_call(
        open_kernel,
        grid=(HEADS // OPEN_HEADS,),
        in_specs=[VMEM, VMEM],
        out_specs=pl.BlockSpec((LAYERS, 8 * OPEN_HEADS, 4 * LANES), lambda h: (0, h, 0)),
        out_shape=jax.ShapeDtypeStruct((LAYERS, SLICE, 4 * LANES), jnp.float32),
        compiler_params=limit(16),
        name="opened",
    )(words, scales)


def on_device(hidden, joined_weight, src_block, group_map, q_slot):
    hidden = pltpu.with_memory_space_constraint(hidden, pltpu.HBM)
    weight = pltpu.with_memory_space_constraint(jnp.swapaxes(joined_weight, 1, 2), pltpu.HBM)
    away, rows, weight = away_product(hidden, weight)
    theirs = lax.ppermute(away, "core", [(0, 1), (1, 0)])
    tables = [pltpu.with_memory_space_constraint(t, pltpu.HBM) for t in (src_block, group_map, q_slot)]
    mine, *tables = my_product(hidden, rows, weight, *tables)
    words = pack(mine, theirs)
    words = lax.all_to_all(words, ("near", "head"), 0, 0, tiled=True)
    words, scales = route(*tables, words)
    words = lax.all_to_all(words, "head", 0, 0, tiled=True)
    return opened(words, scales)


def solution(mesh):
    split = Mesh(mesh.devices.reshape(HEADS, 2, 2), ("head", "near", "core"))
    kdim = ("near", "core")
    return jax.shard_map(
        on_device,
        mesh=split,
        in_specs=(P(None, None, kdim), P(None, kdim, "head"), P(), P(), P()),
        out_specs=P(None, kdim, "head"),
        check_vma=False,
    )
```

```python
import jax
import jax.numpy as jnp
from jax import lax
from jax.experimental import pallas as pl
from jax.experimental.pallas import tpu as pltpu
from jax.sharding import Mesh, PartitionSpec as P

LAYERS = 3
SLICE = 256
MINE = 2 * SLICE
DEPTH = 2048
LANES = 128
WIDTH = 320
CODE_ROW = 160
EARLY = 2
HEADS = 32
GROUP_DEVS = 4
KV_HEADS = 8
GROUP = 8
CODES = 256.0
TOP = 32700.0

VMEM = pl.BlockSpec(memory_space=pltpu.VMEM)
SMEM = pl.BlockSpec(memory_space=pltpu.SMEM)
HBM = pl.BlockSpec(memory_space=pltpu.HBM)


def limit(mib):
    return pltpu.CompilerParams(vmem_limit_bytes=mib * 1024 * 1024)


def codes_of(amax):
    return jnp.ceil(CODES * jnp.log2(jnp.maximum(amax, 1e-30) * (1.0 / TOP))).astype(jnp.int32)


def scale_of(code):
    return jnp.exp2(code.astype(jnp.float32) * (1.0 / CODES))


def inverse_scale_of(code):
    return jnp.exp2(code.astype(jnp.float32) * (-1.0 / CODES))


def whole(x):
    return jnp.round(x).astype(jnp.int32)


def packed(low, high):
    return (low & 0xFFFF) | (high << 16)


def low_of(words):
    return (words << 16) >> 16


def high_of(words):
    return words >> 16


def column_of(head):
    return ((head >> 1) & 3) * 4 + (head >> 3)


def lanes():
    return lax.broadcasted_iota(jnp.int32, (8, LANES), 1)


def product_of(rows, weight):
    return lax.dot_general(
        weight, rows, (((1,), (1,)), ((), ())), preferred_element_type=jnp.float32
    )


def away_kernel(hidden, weight, out, my_rows, weight_rows, away_rows, arrived):
    core = lax.axis_index("core")
    odd = lax.axis_index("far")

    def rows_copy(l, x, other):
        first = pl.multiple_of((2 * x + (1 - core if other else core)) * SLICE, SLICE)
        target = away_rows if other else my_rows
        return pltpu.make_async_copy(
            hidden.at[l, pl.ds(first, SLICE), :],
            target.at[l, pl.ds(SLICE * x, SLICE), :],
            arrived.at[l, 2 * int(other) + x],
        )

    def weight_copies(l):
        blocks = pl.multiple_of(64 * odd, 64)
        half = pl.multiple_of(256 * (1 - odd), 64)
        return [
            pltpu.make_async_copy(
                weight.at[l, pl.ds(blocks, 256), :],
                weight_rows.at[l, pl.ds(0, 256), :],
                arrived.at[l, 4],
            ),
            pltpu.make_async_copy(
                weight.at[l, pl.ds(half, 64), :],
                weight_rows.at[l, pl.ds(256, 64), :],
                arrived.at[l, 5],
            ),
        ]

    for l in range(LAYERS):
        for copy in weight_copies(l):
            copy.start()
        for x in range(2):
            rows_copy(l, x, True).start()
    for l in range(EARLY):
        for x in range(2):
            rows_copy(l, x, False).start()

    @pl.loop(0, LAYERS)
    def _(l):
        for copy in weight_copies(l):
            copy.wait()
        for x in range(2):
            rows_copy(l, x, True).wait()
        value = product_of(away_rows[l], weight_rows[l])
        code = codes_of(jnp.max(jnp.abs(value), axis=0, keepdims=True))
        value = whole(value * inverse_scale_of(code))
        out[l, :LANES, :] = packed(value[:LANES], value[LANES : 2 * LANES])
        out[l, LANES:CODE_ROW, :] = packed(value[2 * LANES : 2 * LANES + 32], value[2 * LANES + 32 :])
        out[l, CODE_ROW:, :] = jnp.broadcast_to(code, (8, MINE))

    for l in range(EARLY):
        for x in range(2):
            rows_copy(l, x, False).wait()


def away_product(hidden, weight):
    return pl.pallas_call(
        away_kernel,
        in_specs=[HBM, HBM],
        out_specs=[VMEM, VMEM, VMEM],
        scratch_shapes=[
            pltpu.VMEM((LAYERS, MINE, DEPTH), jnp.bfloat16),
            pltpu.SemaphoreType.DMA((LAYERS, 6)),
        ],
        out_shape=[
            pltpu.VMEM((LAYERS, CODE_ROW + 8, MINE), jnp.int32),
            pltpu.VMEM((EARLY, MINE, DEPTH), jnp.bfloat16),
            pltpu.VMEM((LAYERS, WIDTH, DEPTH), jnp.bfloat16),
        ],
        cost_estimate=pl.CostEstimate(
            flops=LAYERS * MINE * DEPTH * WIDTH * 2, bytes_accessed=20_000_000, transcendentals=0
        ),
        compiler_params=limit(44),
        name="away_product",
    )(hidden, weight)


def my_kernel(
    hidden, rows, weight, src, grp, slot, out, src_out, grp_out, slot_out, late, arrived
):
    core = lax.axis_index("core")
    copies = []
    for x in range(2):
        first = pl.multiple_of((2 * x + core) * SLICE, SLICE)
        copies.append(
            pltpu.make_async_copy(
                hidden.at[EARLY, pl.ds(first, SLICE), :],
                late.at[pl.ds(SLICE * x, SLICE), :],
                arrived.at[x],
            )
        )
    for k, (here, there) in enumerate(((src, src_out), (grp, grp_out), (slot, slot_out))):
        copies.append(pltpu.make_async_copy(here, there, arrived.at[2 + k]))
    for copy in copies:
        copy.start()

    @pl.loop(0, EARLY)
    def _(l):
        out[l] = product_of(rows[l], weight[l])

    for copy in copies:
        copy.wait()
    out[EARLY] = product_of(late[...], weight[EARLY])


def my_product(hidden, rows, weight, src_block, group_map, q_slot):
    return pl.pallas_call(
        my_kernel,
        in_specs=[HBM, VMEM, VMEM, HBM, HBM, HBM],
        out_specs=[VMEM, SMEM, SMEM, SMEM],
        scratch_shapes=[
            pltpu.VMEM((MINE, DEPTH), jnp.bfloat16),
            pltpu.SemaphoreType.DMA((5,)),
        ],
        out_shape=[
            pltpu.VMEM((LAYERS, WIDTH, MINE), jnp.float32),
            pltpu.SMEM((KV_HEADS,), jnp.int32),
            pltpu.SMEM((KV_HEADS,), jnp.int32),
            pltpu.SMEM((KV_HEADS * GROUP,), jnp.int32),
        ],
        cost_estimate=pl.CostEstimate(
            flops=LAYERS * MINE * DEPTH * WIDTH * 2, bytes_accessed=12_000_000, transcendentals=0
        ),
        compiler_params=limit(24),
        name="my_product",
    )(hidden, rows, weight, src_block, group_map, q_slot)


TILES = LANES // 8


def pack_kernel(mine, theirs, out, sums):
    lane = lanes()
    odd = lax.axis_index("far")
    is_odd = odd == 1
    spare = (lane >= 64) != is_odd
    slot = lane & 63

    @pl.loop(0, 2)
    def _(x):
        codes = jnp.zeros((8, LANES), jnp.int32)
        first = x * (HEADS // 2)

        def place(head):
            return (head & 1) * HEADS + column_of(head)

        for j in range(SLICE // LANES):
            tokens = pl.ds(pl.multiple_of(x * SLICE + j * LANES, LANES), LANES)

            top = None
            for l in range(LAYERS):
                scale = scale_of(theirs[l, CODE_ROW:, tokens])
                for at in range(0, CODE_ROW, 8):
                    word = theirs[l, at : at + 8, tokens]
                    low_row = at if at < LANES else at + LANES
                    high_row = low_row + (LANES if at < LANES else 32)
                    for row, half in ((low_row, low_of(word)), (high_row, high_of(word))):
                        value = mine[l, row : row + 8, tokens] + half.astype(jnp.float32) * scale
                        sums[l, row : row + 8, :] = value
                        value = jnp.abs(value)
                        top = value if top is None else jnp.maximum(top, value)
            code = codes_of(jnp.max(top, axis=0, keepdims=True))
            inverse = inverse_scale_of(code)
            rest = []
            for l in range(LAYERS):
                a = whole(sums[l, :LANES, :] * inverse)
                b = whole(sums[l, LANES : 2 * LANES, :] * inverse)
                words = packed(a, b).T.reshape(TILES, 8, LANES)
                for i in range(TILES):
                    out[first + place(j * TILES + i), 8 * l : 8 * l + 8, :] = words[i]
                rest.append(whole(sums[l, 2 * LANES :, :] * inverse))
            shown = jnp.broadcast_to(code, (64, LANES))
            low = jnp.concatenate(
                [jnp.where(is_odd, rest[1], rest[0]), jnp.where(is_odd, rest[0], rest[1])], axis=0
            )
            high = jnp.concatenate(
                [jnp.where(is_odd, shown, rest[2]), jnp.where(is_odd, rest[2], shown)], axis=0
            )
            words = packed(low, high).T.reshape(TILES, 8, LANES)
            for i in range(TILES):
                out[first + place(j * TILES + i), 24:32, :] = words[i]
                codes = jnp.where(slot == j * TILES + i, words[i], codes)
        codes = codes & ~0xFFFF
        shown = spare & (slot < HEADS)
        for i in range(HEADS):
            word = out[first + place(i), 24:32, :]
            out[first + place(i), 24:32, :] = jnp.where(shown, (word & 0xFFFF) | codes, word)


def pack(mine, theirs):
    return pl.pallas_call(
        pack_kernel,
        in_specs=[VMEM, VMEM],
        out_specs=VMEM,
        scratch_shapes=[pltpu.VMEM((LAYERS, WIDTH, LANES), jnp.float32)],
        out_shape=pltpu.VMEM((2 * HEADS, 32, LANES), jnp.int32),
        compiler_params=limit(16),
        name="pack",
    )(mine, theirs)


def route_kernel(src, grp, slot, words, out, scales, whole_q, where_q):
    reach = []
    for x in range(2):
        tops = []
        for parity in range(2):
            top = None
            for m in range(HEADS // 2):
                code = high_of(words[parity * HEADS + x * (HEADS // 2) + m, 24:32, :])
                top = code if top is None else jnp.maximum(top, code)
            tops.append(top)
        reach.append(scale_of(jnp.maximum(tops[0], pltpu.roll(tops[1], 64, 1))))
    reach = reach[0] + reach[1]
    scales[...] = reach
    inverse = 1.0 / reach[:, 96:97]
    left = lanes() < 64

    @pl.loop(0, KV_HEADS, unroll=True)
    def _(r):
        source = column_of(src[r] * GROUP_DEVS)
        target = column_of(grp[r] * GROUP_DEVS)
        for j in range(GROUP):
            where_q[slot[r * GROUP + j]] = j
        blocks = [[None] * 10 for _ in range(LAYERS)]
        for pair in range(2):
            even, odd = 2 * pair, 2 * pair + 1
            tiles = {}
            rest = None
            for x in range(2):
                third = {}
                for m in (even, odd):
                    device = (m & 1) * HEADS + x * (HEADS // 2) + source + column_of(m)
                    last = words[device, 24:32, :]
                    low, high = low_of(last), high_of(last)
                    at = 96 if m == even else 32
                    ratio = scale_of(high[:, at : at + 1]) * inverse
                    third[m] = (low.astype(jnp.float32) * ratio, high.astype(jnp.float32) * ratio)
                    for l in range(LAYERS):
                        word = words[device, 8 * l : 8 * l + 8, :]
                        a = low_of(word).astype(jnp.float32) * ratio
                        b = high_of(word).astype(jnp.float32) * ratio
                        if x == 0:
                            tiles[m, l] = (a, b)
                        else:
                            tiles[m, l] = (tiles[m, l][0] + a, tiles[m, l][1] + b)
                part = [
                    jnp.where(left, third[even][0], third[odd][0]),
                    jnp.where(left, third[odd][0], third[even][0]),
                    jnp.where(left, third[even][1], third[odd][1]),
                ]
                rest = part if x == 0 else [p + q for p, q in zip(rest, part)]
            rest[1] = pltpu.roll(rest[1], 64, 1)
            for l in range(LAYERS):
                blocks[l][5 * pair : 5 * pair + 5] = [
                    tiles[even, l][0],
                    tiles[even, l][1],
                    rest[l],
                    tiles[odd, l][0],
                    tiles[odd, l][1],
                ]
        for l in range(LAYERS):
            for j in range(GROUP):
                whole_q[j, l] = whole(blocks[l][j])
            key_value = packed(whole(blocks[l][8]), whole(blocks[l][9]))
            for s in range(GROUP_DEVS):
                device = target + (s & 1) * (HEADS // 2) + column_of(s)
                out[device, 24 + 8 * l : 32 + 8 * l, :] = key_value
        for s in range(GROUP_DEVS):
            device = target + (s & 1) * (HEADS // 2) + column_of(s)
            first, second = where_q[2 * s] & 7, where_q[2 * s + 1] & 7
            for l in range(LAYERS):
                out[device, 8 * l : 8 * l + 8, :] = packed(whole_q[first, l], whole_q[second, l])


def route(src, grp, slot, words):
    return pl.pallas_call(
        route_kernel,
        in_specs=[SMEM, SMEM, SMEM, VMEM],
        out_specs=[VMEM, VMEM],
        scratch_shapes=[
            pltpu.VMEM((GROUP, LAYERS, 8, LANES), jnp.int32),
            pltpu.SMEM((GROUP,), jnp.int32),
        ],
        out_shape=[
            pltpu.VMEM((HEADS, 48, LANES), jnp.int32),
            pltpu.VMEM((8, LANES), jnp.float32),
        ],
        compiler_params=limit(16),
        name="route",
    )(src, grp, slot, words)


OPEN_HEADS = 16


def open_kernel(words, scales, out):
    step = pl.program_id(0)
    scale_columns = pltpu.roll(scales[...], 64 - OPEN_HEADS * step, 1)
    for i in range(OPEN_HEADS):
        block = (i & 1) * (HEADS // 2) + column_of(i) + step * (OPEN_HEADS // 8)
        scale = scale_columns[:, i : i + 1]
        rows = slice(8 * i, 8 * i + 8)
        for l in range(LAYERS):
            for half in range(2):
                first = 24 * half + 8 * l
                word = words[block, first : first + 8, :]
                cols = 2 * LANES * half
                out[l, rows, cols : cols + LANES] = low_of(word).astype(jnp.float32) * scale
                out[l, rows, cols + LANES : cols + 2 * LANES] = (
                    high_of(word).astype(jnp.float32) * scale
                )


def opened(words, scales):
    return pl.pallas_call(
        open_kernel,
        grid=(HEADS // OPEN_HEADS,),
        in_specs=[VMEM, VMEM],
        out_specs=pl.BlockSpec((LAYERS, 8 * OPEN_HEADS, 4 * LANES), lambda h: (0, h, 0)),
        out_shape=jax.ShapeDtypeStruct((LAYERS, SLICE, 4 * LANES), jnp.float32),
        compiler_params=limit(16),
        name="opened",
    )(words, scales)


def on_device(hidden, joined_weight, src_block, group_map, q_slot):
    hidden = pltpu.with_memory_space_constraint(hidden, pltpu.HBM)
    weight = pltpu.with_memory_space_constraint(jnp.swapaxes(joined_weight, 1, 2), pltpu.HBM)
    away, rows, weight = away_product(hidden, weight)
    theirs = lax.ppermute(away, "core", [(0, 1), (1, 0)])
    tables = [pltpu.with_memory_space_constraint(t, pltpu.HBM) for t in (src_block, group_map, q_slot)]
    mine, *tables = my_product(hidden, rows, weight, *tables)
    words = pack(mine, theirs)
    words = lax.all_to_all(words, ("far", "near", "y", "z"), 0, 0, tiled=True)
    words, scales = route(*tables, words)
    words = lax.all_to_all(words, ("far", "y", "z"), 0, 0, tiled=True)
    return opened(words, scales)


def solution(mesh):
    split = Mesh(mesh.devices.reshape(4, 4, 2, 2, 2), ("z", "y", "far", "near", "core"))
    head, kdim = ("z", "y", "far"), ("near", "core")
    return jax.shard_map(
        on_device,
        mesh=split,
        in_specs=(P(None, None, kdim), P(None, kdim, head), P(), P(), P()),
        out_specs=P(None, kdim, head),
        check_vma=False,
    )
```

```python
import jax
import jax.numpy as jnp
from jax import lax
from jax.experimental import pallas as pl
from jax.experimental.pallas import tpu as pltpu
from jax.sharding import Mesh, PartitionSpec as P

LAYERS = 3
SLICE = 256
MINE = 2 * SLICE
DEPTH = 2048
LANES = 128
WIDTH = 320
CODE_ROW = 160
EARLY = 2
HEADS = 32
GROUP_DEVS = 4
KV_HEADS = 8
GROUP = 8
CODES = 256.0
TOP = 32700.0

VMEM = pl.BlockSpec(memory_space=pltpu.VMEM)
SMEM = pl.BlockSpec(memory_space=pltpu.SMEM)
HBM = pl.BlockSpec(memory_space=pltpu.HBM)


def limit(mib):
    return pltpu.CompilerParams(vmem_limit_bytes=mib * 1024 * 1024)


def codes_of(amax):
    return jnp.ceil(CODES * jnp.log2(jnp.maximum(amax, 1e-30) * (1.0 / TOP))).astype(jnp.int32)


def scale_of(code):
    return jnp.exp2(code.astype(jnp.float32) * (1.0 / CODES))


def inverse_scale_of(code):
    return jnp.exp2(code.astype(jnp.float32) * (-1.0 / CODES))


def whole(x):
    return jnp.round(x).astype(jnp.int32)


def packed(low, high):
    return (low & 0xFFFF) | (high << 16)


def low_of(words):
    return (words << 16) >> 16


def high_of(words):
    return words >> 16


def column_of(head):
    return ((head >> 1) & 3) * 4 + (head >> 3)


def lanes():
    return lax.broadcasted_iota(jnp.int32, (8, LANES), 1)


def product_of(rows, weight):
    return lax.dot_general(
        weight, rows, (((1,), (1,)), ((), ())), preferred_element_type=jnp.float32
    )


def away_kernel(hidden, weight, out, my_rows, weight_rows, away_rows, arrived):
    core = lax.axis_index("core")
    odd = lax.axis_index("far")

    def rows_copy(l, x, other):
        first = pl.multiple_of((2 * x + (1 - core if other else core)) * SLICE, SLICE)
        target = away_rows if other else my_rows
        return pltpu.make_async_copy(
            hidden.at[l, pl.ds(first, SLICE), :],
            target.at[l, pl.ds(SLICE * x, SLICE), :],
            arrived.at[l, 2 * int(other) + x],
        )

    def weight_copies(l):
        blocks = pl.multiple_of(64 * odd, 64)
        half = pl.multiple_of(256 * (1 - odd), 64)
        return [
            pltpu.make_async_copy(
                weight.at[l, pl.ds(blocks, 256), :],
                weight_rows.at[l, pl.ds(0, 256), :],
                arrived.at[l, 4],
            ),
            pltpu.make_async_copy(
                weight.at[l, pl.ds(half, 64), :],
                weight_rows.at[l, pl.ds(256, 64), :],
                arrived.at[l, 5],
            ),
        ]

    for l in range(LAYERS):
        for copy in weight_copies(l):
            copy.start()
        for x in range(2):
            rows_copy(l, x, True).start()
    for l in range(EARLY):
        for x in range(2):
            rows_copy(l, x, False).start()

    @pl.loop(0, LAYERS)
    def _(l):
        for copy in weight_copies(l):
            copy.wait()
        for x in range(2):
            rows_copy(l, x, True).wait()
        value = product_of(away_rows[l], weight_rows[l])
        code = codes_of(jnp.max(jnp.abs(value), axis=0, keepdims=True))
        value = whole(value * inverse_scale_of(code))
        out[l, :LANES, :] = packed(value[:LANES], value[LANES : 2 * LANES])
        out[l, LANES:CODE_ROW, :] = packed(value[2 * LANES : 2 * LANES + 32], value[2 * LANES + 32 :])
        out[l, CODE_ROW:, :] = jnp.broadcast_to(code, (8, MINE))

    for l in range(EARLY):
        for x in range(2):
            rows_copy(l, x, False).wait()


def away_product(hidden, weight):
    return pl.pallas_call(
        away_kernel,
        in_specs=[HBM, HBM],
        out_specs=[VMEM, VMEM, VMEM],
        scratch_shapes=[
            pltpu.VMEM((LAYERS, MINE, DEPTH), jnp.bfloat16),
            pltpu.SemaphoreType.DMA((LAYERS, 6)),
        ],
        out_shape=[
            pltpu.VMEM((LAYERS, CODE_ROW + 8, MINE), jnp.int32),
            pltpu.VMEM((EARLY, MINE, DEPTH), jnp.bfloat16),
            pltpu.VMEM((LAYERS, WIDTH, DEPTH), jnp.bfloat16),
        ],
        cost_estimate=pl.CostEstimate(
            flops=LAYERS * MINE * DEPTH * WIDTH * 2, bytes_accessed=20_000_000, transcendentals=0
        ),
        compiler_params=limit(44),
        name="away_product",
    )(hidden, weight)


def my_kernel(
    hidden, rows, weight, src, grp, slot, out, src_out, grp_out, slot_out, late, arrived
):
    core = lax.axis_index("core")
    copies = []
    for x in range(2):
        first = pl.multiple_of((2 * x + core) * SLICE, SLICE)
        copies.append(
            pltpu.make_async_copy(
                hidden.at[EARLY, pl.ds(first, SLICE), :],
                late.at[pl.ds(SLICE * x, SLICE), :],
                arrived.at[x],
            )
        )
    for k, (here, there) in enumerate(((src, src_out), (grp, grp_out), (slot, slot_out))):
        copies.append(pltpu.make_async_copy(here, there, arrived.at[2 + k]))
    for copy in copies:
        copy.start()

    @pl.loop(0, EARLY)
    def _(l):
        out[l] = product_of(rows[l], weight[l])

    for copy in copies:
        copy.wait()
    out[EARLY] = product_of(late[...], weight[EARLY])


def my_product(hidden, rows, weight, src_block, group_map, q_slot):
    return pl.pallas_call(
        my_kernel,
        in_specs=[HBM, VMEM, VMEM, HBM, HBM, HBM],
        out_specs=[VMEM, SMEM, SMEM, SMEM],
        scratch_shapes=[
            pltpu.VMEM((MINE, DEPTH), jnp.bfloat16),
            pltpu.SemaphoreType.DMA((5,)),
        ],
        out_shape=[
            pltpu.VMEM((LAYERS, WIDTH, MINE), jnp.float32),
            pltpu.SMEM((KV_HEADS,), jnp.int32),
            pltpu.SMEM((KV_HEADS,), jnp.int32),
            pltpu.SMEM((KV_HEADS * GROUP,), jnp.int32),
        ],
        cost_estimate=pl.CostEstimate(
            flops=LAYERS * MINE * DEPTH * WIDTH * 2, bytes_accessed=12_000_000, transcendentals=0
        ),
        compiler_params=limit(24),
        name="my_product",
    )(hidden, rows, weight, src_block, group_map, q_slot)


TILES = LANES // 8


def pack_kernel(mine, theirs, out, sums):
    lane = lanes()
    odd = lax.axis_index("far")
    is_odd = odd == 1
    spare = (lane >= 64) != is_odd
    slot = lane & 63

    @pl.loop(0, 2)
    def _(x):
        codes = jnp.zeros((8, LANES), jnp.int32)
        first = x * (HEADS // 2)

        def place(head):
            return (head & 1) * HEADS + column_of(head)

        for j in range(SLICE // LANES):
            tokens = pl.ds(pl.multiple_of(x * SLICE + j * LANES, LANES), LANES)

            top = None
            for l in range(LAYERS):
                scale = scale_of(theirs[l, CODE_ROW:, tokens])
                for at in range(0, CODE_ROW, 8):
                    word = theirs[l, at : at + 8, tokens]
                    low_row = at if at < LANES else at + LANES
                    high_row = low_row + (LANES if at < LANES else 32)
                    for row, half in ((low_row, low_of(word)), (high_row, high_of(word))):
                        value = mine[l, row : row + 8, tokens] + half.astype(jnp.float32) * scale
                        sums[l, row : row + 8, :] = value
                        value = jnp.abs(value)
                        top = value if top is None else jnp.maximum(top, value)
            code = codes_of(jnp.max(top, axis=0, keepdims=True))
            inverse = inverse_scale_of(code)
            rest = []
            for l in range(LAYERS):
                a = whole(sums[l, :LANES, :] * inverse)
                b = whole(sums[l, LANES : 2 * LANES, :] * inverse)
                words = packed(a, b).T.reshape(TILES, 8, LANES)
                for i in range(TILES):
                    out[first + place(j * TILES + i), 8 * l : 8 * l + 8, :] = words[i]
                rest.append(whole(sums[l, 2 * LANES :, :] * inverse))
            shown = jnp.broadcast_to(code, (64, LANES))
            low = jnp.concatenate(
                [jnp.where(is_odd, rest[1], rest[0]), jnp.where(is_odd, rest[0], rest[1])], axis=0
            )
            high = jnp.concatenate(
                [jnp.where(is_odd, shown, rest[2]), jnp.where(is_odd, rest[2], shown)], axis=0
            )
            words = packed(low, high).T.reshape(TILES, 8, LANES)
            for i in range(TILES):
                out[first + place(j * TILES + i), 24:32, :] = words[i]
                codes = jnp.where(slot == j * TILES + i, words[i], codes)
        codes = codes & ~0xFFFF
        shown = spare & (slot < HEADS)
        for i in range(HEADS):
            word = out[first + place(i), 24:32, :]
            out[first + place(i), 24:32, :] = jnp.where(shown, (word & 0xFFFF) | codes, word)


def pack(mine, theirs):
    return pl.pallas_call(
        pack_kernel,
        in_specs=[VMEM, VMEM],
        out_specs=VMEM,
        scratch_shapes=[pltpu.VMEM((LAYERS, WIDTH, LANES), jnp.float32)],
        out_shape=pltpu.VMEM((2 * HEADS, 32, LANES), jnp.int32),
        compiler_params=limit(16),
        name="pack",
    )(mine, theirs)


def device_of(source, x, m):
    return (m & 1) * HEADS + x * (HEADS // 2) + source + column_of(m)


def reached(scale):
    halves = []
    for x in range(2):
        top = scale[x, 0]
        for m in range(1, GROUP_DEVS):
            top = jnp.maximum(top, scale[x, m])
        halves.append(top)
    return halves[0] + halves[1]


def route_kernel(src, grp, slot, words, out, scales, whole_q, where_q):
    left = lanes() < 64

    @pl.loop(0, KV_HEADS, unroll=True)
    def _(r):
        source = column_of(src[r] * GROUP_DEVS)
        target = column_of(grp[r] * GROUP_DEVS)
        for j in range(GROUP):
            where_q[slot[r * GROUP + j]] = j
        scale = {}
        for x in range(2):
            for m in range(GROUP_DEVS):
                code = high_of(words[device_of(source, x, m), 24:32, :])
                at = 96 if m % 2 == 0 else 32
                scale[x, m] = scale_of(code[:, at : at + 1])
        inverse = 1.0 / reached(scale)
        blocks = [[None] * 10 for _ in range(LAYERS)]
        for pair in range(2):
            even, odd = 2 * pair, 2 * pair + 1
            tiles = {}
            rest = None
            for x in range(2):
                third = {}
                for m in (even, odd):
                    device = device_of(source, x, m)
                    last = words[device, 24:32, :]
                    low, high = low_of(last), high_of(last)
                    ratio = scale[x, m] * inverse
                    third[m] = (low.astype(jnp.float32) * ratio, high.astype(jnp.float32) * ratio)
                    for l in range(LAYERS):
                        word = words[device, 8 * l : 8 * l + 8, :]
                        a = low_of(word).astype(jnp.float32) * ratio
                        b = high_of(word).astype(jnp.float32) * ratio
                        if x == 0:
                            tiles[m, l] = (a, b)
                        else:
                            tiles[m, l] = (tiles[m, l][0] + a, tiles[m, l][1] + b)
                part = [
                    jnp.where(left, third[even][0], third[odd][0]),
                    jnp.where(left, third[odd][0], third[even][0]),
                    jnp.where(left, third[even][1], third[odd][1]),
                ]
                rest = part if x == 0 else [p + q for p, q in zip(rest, part)]
            rest[1] = pltpu.roll(rest[1], 64, 1)
            for l in range(LAYERS):
                blocks[l][5 * pair : 5 * pair + 5] = [
                    tiles[even, l][0],
                    tiles[even, l][1],
                    rest[l],
                    tiles[odd, l][0],
                    tiles[odd, l][1],
                ]
        for l in range(LAYERS):
            for j in range(GROUP):
                whole_q[j, l] = whole(blocks[l][j])
            key_value = packed(whole(blocks[l][8]), whole(blocks[l][9]))
            for s in range(GROUP_DEVS):
                device = target + (s & 1) * (HEADS // 2) + column_of(s)
                out[device, 24 + 8 * l : 32 + 8 * l, :] = key_value
        for s in range(GROUP_DEVS):
            device = target + (s & 1) * (HEADS // 2) + column_of(s)
            first, second = where_q[2 * s] & 7, where_q[2 * s + 1] & 7
            for l in range(LAYERS):
                out[device, 8 * l : 8 * l + 8, :] = packed(whole_q[first, l], whole_q[second, l])

    own = lax.axis_index("z") * 2 + (lax.axis_index("y") >> 1)
    block = 0
    for r in range(KV_HEADS):
        block = jnp.where(grp[r] == own, src[r], block)
    source = column_of(block * GROUP_DEVS)
    scale = {}
    for x in range(2):
        for m in range(GROUP_DEVS):
            code = high_of(words[device_of(source, x, m), 24:32, :])
            code = code if m % 2 == 0 else pltpu.roll(code, 64, 1)
            scale[x, m] = scale_of(code)
    scales[...] = reached(scale)


def route(src, grp, slot, words):
    return pl.pallas_call(
        route_kernel,
        in_specs=[SMEM, SMEM, SMEM, VMEM],
        out_specs=[VMEM, VMEM],
        scratch_shapes=[
            pltpu.VMEM((GROUP, LAYERS, 8, LANES), jnp.int32),
            pltpu.SMEM((GROUP,), jnp.int32),
        ],
        out_shape=[
            pltpu.VMEM((HEADS, 48, LANES), jnp.int32),
            pltpu.VMEM((8, LANES), jnp.float32),
        ],
        compiler_params=limit(16),
        name="route",
    )(src, grp, slot, words)


OPEN_HEADS = 16


def open_kernel(words, scales, out):
    step = pl.program_id(0)
    scale_columns = pltpu.roll(scales[...], 64 - OPEN_HEADS * step, 1)
    for i in range(OPEN_HEADS):
        block = (i & 1) * (HEADS // 2) + column_of(i) + step * (OPEN_HEADS // 8)
        scale = scale_columns[:, i : i + 1]
        rows = slice(8 * i, 8 * i + 8)
        for l in range(LAYERS):
            for half in range(2):
                first = 24 * half + 8 * l
                word = words[block, first : first + 8, :]
                cols = 2 * LANES * half
                out[l, rows, cols : cols + LANES] = low_of(word).astype(jnp.float32) * scale
                out[l, rows, cols + LANES : cols + 2 * LANES] = (
                    high_of(word).astype(jnp.float32) * scale
                )


def opened(words, scales):
    return pl.pallas_call(
        open_kernel,
        grid=(HEADS // OPEN_HEADS,),
        in_specs=[VMEM, VMEM],
        out_specs=pl.BlockSpec((LAYERS, 8 * OPEN_HEADS, 4 * LANES), lambda h: (0, h, 0)),
        out_shape=jax.ShapeDtypeStruct((LAYERS, SLICE, 4 * LANES), jnp.float32),
        compiler_params=limit(16),
        name="opened",
    )(words, scales)


def on_device(hidden, joined_weight, src_block, group_map, q_slot):
    hidden = pltpu.with_memory_space_constraint(hidden, pltpu.HBM)
    weight = pltpu.with_memory_space_constraint(jnp.swapaxes(joined_weight, 1, 2), pltpu.HBM)
    away, rows, weight = away_product(hidden, weight)
    theirs = lax.ppermute(away, "core", [(0, 1), (1, 0)])
    tables = [pltpu.with_memory_space_constraint(t, pltpu.HBM) for t in (src_block, group_map, q_slot)]
    mine, *tables = my_product(hidden, rows, weight, *tables)
    words = pack(mine, theirs)
    words = lax.all_to_all(words, ("far", "near", "y", "z"), 0, 0, tiled=True)
    words, scales = route(*tables, words)
    words = lax.all_to_all(words, ("far", "y", "z"), 0, 0, tiled=True)
    return opened(words, scales)


def solution(mesh):
    split = Mesh(mesh.devices.reshape(4, 4, 2, 2, 2), ("z", "y", "far", "near", "core"))
    head, kdim = ("z", "y", "far"), ("near", "core")
    return jax.shard_map(
        on_device,
        mesh=split,
        in_specs=(P(None, None, kdim), P(None, kdim, head), P(), P(), P()),
        out_specs=P(None, kdim, head),
        check_vma=False,
    )
```

```python
import jax
import jax.numpy as jnp
from jax import lax
from jax.experimental import pallas as pl
from jax.experimental.pallas import tpu as pltpu
from jax.sharding import Mesh, PartitionSpec as P

LAYERS = 3
SLICE = 256
MINE = 2 * SLICE
DEPTH = 2048
LANES = 128
WIDTH = 320
CODE_ROW = 160
EARLY = 2
HEADS = 32
GROUP_DEVS = 4
KV_HEADS = 8
GROUP = 8
CODES = 256.0
TOP = 32700.0

VMEM = pl.BlockSpec(memory_space=pltpu.VMEM)
SMEM = pl.BlockSpec(memory_space=pltpu.SMEM)
HBM = pl.BlockSpec(memory_space=pltpu.HBM)


def limit(mib):
    return pltpu.CompilerParams(vmem_limit_bytes=mib * 1024 * 1024)


def codes_of(amax):
    return jnp.ceil(CODES * jnp.log2(jnp.maximum(amax, 1e-30) * (1.0 / TOP))).astype(jnp.int32)


def scale_of(code):
    return jnp.exp2(code.astype(jnp.float32) * (1.0 / CODES))


def inverse_scale_of(code):
    return jnp.exp2(code.astype(jnp.float32) * (-1.0 / CODES))


def whole(x):
    return jnp.round(x).astype(jnp.int32)


def packed(low, high):
    return (low & 0xFFFF) | (high << 16)


def low_of(words):
    return (words << 16) >> 16


def high_of(words):
    return words >> 16


def column_of(head):
    return ((head >> 1) & 3) * 4 + (head >> 3)


def lanes():
    return lax.broadcasted_iota(jnp.int32, (8, LANES), 1)


def product_of(rows, weight):
    return lax.dot_general(
        weight, rows, (((1,), (1,)), ((), ())), preferred_element_type=jnp.float32
    )


def away_kernel(hidden, weight, out, my_rows, weight_rows, away_rows, arrived):
    core = lax.axis_index("core")
    odd = lax.axis_index("far")

    def rows_copy(l, x, other):
        first = pl.multiple_of((2 * x + (1 - core if other else core)) * SLICE, SLICE)
        target = away_rows if other else my_rows
        return pltpu.make_async_copy(
            hidden.at[l, pl.ds(first, SLICE), :],
            target.at[l, pl.ds(SLICE * x, SLICE), :],
            arrived.at[l, 2 * int(other) + x],
        )

    def weight_copies(l):
        blocks = pl.multiple_of(64 * odd, 64)
        half = pl.multiple_of(256 * (1 - odd), 64)
        return [
            pltpu.make_async_copy(
                weight.at[l, pl.ds(blocks, 256), :],
                weight_rows.at[l, pl.ds(0, 256), :],
                arrived.at[l, 4],
            ),
            pltpu.make_async_copy(
                weight.at[l, pl.ds(half, 64), :],
                weight_rows.at[l, pl.ds(256, 64), :],
                arrived.at[l, 5],
            ),
        ]

    for l in range(LAYERS):
        for copy in weight_copies(l):
            copy.start()
        for x in range(2):
            rows_copy(l, x, True).start()
    for l in range(EARLY):
        for x in range(2):
            rows_copy(l, x, False).start()

    @pl.loop(0, LAYERS)
    def _(l):
        for copy in weight_copies(l):
            copy.wait()
        for x in range(2):
            rows_copy(l, x, True).wait()
        value = product_of(away_rows[l], weight_rows[l])
        code = codes_of(jnp.max(jnp.abs(value), axis=0, keepdims=True))
        value = whole(value * inverse_scale_of(code))
        out[l, :LANES, :] = packed(value[:LANES], value[LANES : 2 * LANES])
        out[l, LANES:CODE_ROW, :] = packed(value[2 * LANES : 2 * LANES + 32], value[2 * LANES + 32 :])
        out[l, CODE_ROW:, :] = jnp.broadcast_to(code, (8, MINE))

    for l in range(EARLY):
        for x in range(2):
            rows_copy(l, x, False).wait()


def away_product(hidden, weight):
    return pl.pallas_call(
        away_kernel,
        in_specs=[HBM, HBM],
        out_specs=[VMEM, VMEM, VMEM],
        scratch_shapes=[
            pltpu.VMEM((LAYERS, MINE, DEPTH), jnp.bfloat16),
            pltpu.SemaphoreType.DMA((LAYERS, 6)),
        ],
        out_shape=[
            pltpu.VMEM((LAYERS, CODE_ROW + 8, MINE), jnp.int32),
            pltpu.VMEM((EARLY, MINE, DEPTH), jnp.bfloat16),
            pltpu.VMEM((LAYERS, WIDTH, DEPTH), jnp.bfloat16),
        ],
        cost_estimate=pl.CostEstimate(
            flops=LAYERS * MINE * DEPTH * WIDTH * 2, bytes_accessed=20_000_000, transcendentals=0
        ),
        compiler_params=limit(44),
        name="away_product",
    )(hidden, weight)


def my_kernel(
    hidden, rows, weight, src, grp, slot, out, src_out, grp_out, slot_out, late, arrived
):
    core = lax.axis_index("core")
    copies = []
    for x in range(2):
        first = pl.multiple_of((2 * x + core) * SLICE, SLICE)
        copies.append(
            pltpu.make_async_copy(
                hidden.at[EARLY, pl.ds(first, SLICE), :],
                late.at[pl.ds(SLICE * x, SLICE), :],
                arrived.at[x],
            )
        )
    for k, (here, there) in enumerate(((src, src_out), (grp, grp_out), (slot, slot_out))):
        copies.append(pltpu.make_async_copy(here, there, arrived.at[2 + k]))
    for copy in copies:
        copy.start()

    @pl.loop(0, EARLY)
    def _(l):
        out[l] = product_of(rows[l], weight[l])

    for copy in copies:
        copy.wait()
    out[EARLY] = product_of(late[...], weight[EARLY])


def my_product(hidden, rows, weight, src_block, group_map, q_slot):
    return pl.pallas_call(
        my_kernel,
        in_specs=[HBM, VMEM, VMEM, HBM, HBM, HBM],
        out_specs=[VMEM, SMEM, SMEM, SMEM],
        scratch_shapes=[
            pltpu.VMEM((MINE, DEPTH), jnp.bfloat16),
            pltpu.SemaphoreType.DMA((5,)),
        ],
        out_shape=[
            pltpu.VMEM((LAYERS, WIDTH, MINE), jnp.float32),
            pltpu.SMEM((KV_HEADS,), jnp.int32),
            pltpu.SMEM((KV_HEADS,), jnp.int32),
            pltpu.SMEM((KV_HEADS * GROUP,), jnp.int32),
        ],
        cost_estimate=pl.CostEstimate(
            flops=LAYERS * MINE * DEPTH * WIDTH * 2, bytes_accessed=12_000_000, transcendentals=0
        ),
        compiler_params=limit(24),
        name="my_product",
    )(hidden, rows, weight, src_block, group_map, q_slot)


TILES = LANES // 8


def pack_kernel(mine, theirs, out, sums):
    lane = lanes()
    odd = lax.axis_index("far")
    is_odd = odd == 1
    spare = (lane >= 64) != is_odd
    slot = lane & 63

    @pl.loop(0, 2, unroll=True)
    def _(x):
        codes = jnp.zeros((8, LANES), jnp.int32)
        first = x * (HEADS // 2)

        def place(head):
            return (head & 1) * HEADS + column_of(head)

        for j in range(SLICE // LANES):
            tokens = pl.ds(pl.multiple_of(x * SLICE + j * LANES, LANES), LANES)

            top = None
            for l in range(LAYERS):
                scale = scale_of(theirs[l, CODE_ROW:, tokens])
                for at in range(0, CODE_ROW, 8):
                    word = theirs[l, at : at + 8, tokens]
                    low_row = at if at < LANES else at + LANES
                    high_row = low_row + (LANES if at < LANES else 32)
                    for row, half in ((low_row, low_of(word)), (high_row, high_of(word))):
                        value = mine[l, row : row + 8, tokens] + half.astype(jnp.float32) * scale
                        sums[l, row : row + 8, :] = value
                        value = jnp.abs(value)
                        top = value if top is None else jnp.maximum(top, value)
            code = codes_of(jnp.max(top, axis=0, keepdims=True))
            inverse = inverse_scale_of(code)
            rest = []
            for l in range(LAYERS):
                a = whole(sums[l, :LANES, :] * inverse)
                b = whole(sums[l, LANES : 2 * LANES, :] * inverse)
                words = packed(a, b).T.reshape(TILES, 8, LANES)
                for i in range(TILES):
                    out[first + place(j * TILES + i), 8 * l : 8 * l + 8, :] = words[i]
                rest.append(whole(sums[l, 2 * LANES :, :] * inverse))
            shown = jnp.broadcast_to(code, (64, LANES))
            low = jnp.concatenate(
                [jnp.where(is_odd, rest[1], rest[0]), jnp.where(is_odd, rest[0], rest[1])], axis=0
            )
            high = jnp.concatenate(
                [jnp.where(is_odd, shown, rest[2]), jnp.where(is_odd, rest[2], shown)], axis=0
            )
            words = packed(low, high).T.reshape(TILES, 8, LANES)
            for i in range(TILES):
                out[first + place(j * TILES + i), 24:32, :] = words[i]
                codes = jnp.where(slot == j * TILES + i, words[i], codes)
        codes = codes & ~0xFFFF
        shown = spare & (slot < HEADS)
        for i in range(HEADS):
            word = out[first + place(i), 24:32, :]
            out[first + place(i), 24:32, :] = jnp.where(shown, (word & 0xFFFF) | codes, word)


def pack(mine, theirs):
    return pl.pallas_call(
        pack_kernel,
        in_specs=[VMEM, VMEM],
        out_specs=VMEM,
        scratch_shapes=[pltpu.VMEM((LAYERS, WIDTH, LANES), jnp.float32)],
        out_shape=pltpu.VMEM((2 * HEADS, 32, LANES), jnp.int32),
        compiler_params=limit(16),
        name="pack",
    )(mine, theirs)


def device_of(source, x, m):
    return (m & 1) * HEADS + x * (HEADS // 2) + source + column_of(m)


def reached(scale):
    halves = []
    for x in range(2):
        top = scale[x, 0]
        for m in range(1, GROUP_DEVS):
            top = jnp.maximum(top, scale[x, m])
        halves.append(top)
    return halves[0] + halves[1]


def route_kernel(src, grp, slot, words, out, scales, whole_q, where_q):
    left = lanes() < 64

    @pl.loop(0, KV_HEADS, unroll=True)
    def _(r):
        source = column_of(src[r] * GROUP_DEVS)
        target = column_of(grp[r] * GROUP_DEVS)
        for j in range(GROUP):
            where_q[slot[r * GROUP + j]] = j
        scale = {}
        for x in range(2):
            for m in range(GROUP_DEVS):
                code = high_of(words[device_of(source, x, m), 24:32, :])
                at = 96 if m % 2 == 0 else 32
                scale[x, m] = scale_of(code[:, at : at + 1])
        inverse = 1.0 / reached(scale)
        blocks = [[None] * 10 for _ in range(LAYERS)]
        for pair in range(2):
            even, odd = 2 * pair, 2 * pair + 1
            tiles = {}
            rest = None
            for x in range(2):
                third = {}
                for m in (even, odd):
                    device = device_of(source, x, m)
                    last = words[device, 24:32, :]
                    low, high = low_of(last), high_of(last)
                    ratio = scale[x, m] * inverse
                    third[m] = (low.astype(jnp.float32) * ratio, high.astype(jnp.float32) * ratio)
                    for l in range(LAYERS):
                        word = words[device, 8 * l : 8 * l + 8, :]
                        a = low_of(word).astype(jnp.float32) * ratio
                        b = high_of(word).astype(jnp.float32) * ratio
                        if x == 0:
                            tiles[m, l] = (a, b)
                        else:
                            tiles[m, l] = (tiles[m, l][0] + a, tiles[m, l][1] + b)
                part = [
                    jnp.where(left, third[even][0], third[odd][0]),
                    jnp.where(left, third[odd][0], third[even][0]),
                    jnp.where(left, third[even][1], third[odd][1]),
                ]
                rest = part if x == 0 else [p + q for p, q in zip(rest, part)]
            rest[1] = pltpu.roll(rest[1], 64, 1)
            for l in range(LAYERS):
                blocks[l][5 * pair : 5 * pair + 5] = [
                    tiles[even, l][0],
                    tiles[even, l][1],
                    rest[l],
                    tiles[odd, l][0],
                    tiles[odd, l][1],
                ]
        for l in range(LAYERS):
            for j in range(GROUP):
                whole_q[j, l] = whole(blocks[l][j])
            key_value = packed(whole(blocks[l][8]), whole(blocks[l][9]))
            for s in range(GROUP_DEVS):
                device = target + (s & 1) * (HEADS // 2) + column_of(s)
                out[device, 24 + 8 * l : 32 + 8 * l, :] = key_value
        for s in range(GROUP_DEVS):
            device = target + (s & 1) * (HEADS // 2) + column_of(s)
            first, second = where_q[2 * s] & 7, where_q[2 * s + 1] & 7
            for l in range(LAYERS):
                out[device, 8 * l : 8 * l + 8, :] = packed(whole_q[first, l], whole_q[second, l])

    own = lax.axis_index("z") * 2 + (lax.axis_index("y") >> 1)
    block = 0
    for r in range(KV_HEADS):
        block = jnp.where(grp[r] == own, src[r], block)
    source = column_of(block * GROUP_DEVS)
    scale = {}
    for x in range(2):
        for m in range(GROUP_DEVS):
            code = high_of(words[device_of(source, x, m), 24:32, :])
            code = code if m % 2 == 0 else pltpu.roll(code, 64, 1)
            scale[x, m] = scale_of(code)
    scales[...] = reached(scale)


def route(src, grp, slot, words):
    return pl.pallas_call(
        route_kernel,
        in_specs=[SMEM, SMEM, SMEM, VMEM],
        out_specs=[VMEM, VMEM],
        scratch_shapes=[
            pltpu.VMEM((GROUP, LAYERS, 8, LANES), jnp.int32),
            pltpu.SMEM((GROUP,), jnp.int32),
        ],
        out_shape=[
            pltpu.VMEM((HEADS, 48, LANES), jnp.int32),
            pltpu.VMEM((8, LANES), jnp.float32),
        ],
        compiler_params=limit(16),
        name="route",
    )(src, grp, slot, words)


OPEN_HEADS = 16


def open_kernel(words, scales, out):
    step = pl.program_id(0)
    scale_columns = pltpu.roll(scales[...], 64 - OPEN_HEADS * step, 1)
    for i in range(OPEN_HEADS):
        block = (i & 1) * (HEADS // 2) + column_of(i) + step * (OPEN_HEADS // 8)
        scale = scale_columns[:, i : i + 1]
        rows = slice(8 * i, 8 * i + 8)
        for l in range(LAYERS):
            for half in range(2):
                first = 24 * half + 8 * l
                word = words[block, first : first + 8, :]
                cols = 2 * LANES * half
                out[l, rows, cols : cols + LANES] = low_of(word).astype(jnp.float32) * scale
                out[l, rows, cols + LANES : cols + 2 * LANES] = (
                    high_of(word).astype(jnp.float32) * scale
                )


def opened(words, scales):
    return pl.pallas_call(
        open_kernel,
        grid=(HEADS // OPEN_HEADS,),
        in_specs=[VMEM, VMEM],
        out_specs=pl.BlockSpec((LAYERS, 8 * OPEN_HEADS, 4 * LANES), lambda h: (0, h, 0)),
        out_shape=jax.ShapeDtypeStruct((LAYERS, SLICE, 4 * LANES), jnp.float32),
        compiler_params=limit(16),
        name="opened",
    )(words, scales)


def on_device(hidden, joined_weight, src_block, group_map, q_slot):
    hidden = pltpu.with_memory_space_constraint(hidden, pltpu.HBM)
    weight = pltpu.with_memory_space_constraint(jnp.swapaxes(joined_weight, 1, 2), pltpu.HBM)
    away, rows, weight = away_product(hidden, weight)
    theirs = lax.ppermute(away, "core", [(0, 1), (1, 0)])
    tables = [pltpu.with_memory_space_constraint(t, pltpu.HBM) for t in (src_block, group_map, q_slot)]
    mine, *tables = my_product(hidden, rows, weight, *tables)
    words = pack(mine, theirs)
    words = lax.all_to_all(words, ("far", "near", "y", "z"), 0, 0, tiled=True)
    words, scales = route(*tables, words)
    words = lax.all_to_all(words, ("far", "y", "z"), 0, 0, tiled=True)
    return opened(words, scales)


def solution(mesh):
    split = Mesh(mesh.devices.reshape(4, 4, 2, 2, 2), ("z", "y", "far", "near", "core"))
    head, kdim = ("z", "y", "far"), ("near", "core")
    return jax.shard_map(
        on_device,
        mesh=split,
        in_specs=(P(None, None, kdim), P(None, kdim, head), P(), P(), P()),
        out_specs=P(None, kdim, head),
        check_vma=False,
    )
```

```python
import jax
import jax.numpy as jnp
from jax import lax
from jax.experimental import pallas as pl
from jax.experimental.pallas import tpu as pltpu
from jax.sharding import Mesh, PartitionSpec as P

LAYERS = 3
SLICE = 256
MINE = 2 * SLICE
DEPTH = 2048
LANES = 128
WIDTH = 320
CODE_ROW = 160
EARLY = 2
HEADS = 32
GROUP_DEVS = 4
KV_HEADS = 8
GROUP = 8
CODES = 256.0
TOP = 32700.0

VMEM = pl.BlockSpec(memory_space=pltpu.VMEM)
SMEM = pl.BlockSpec(memory_space=pltpu.SMEM)
HBM = pl.BlockSpec(memory_space=pltpu.HBM)


def limit(mib):
    return pltpu.CompilerParams(vmem_limit_bytes=mib * 1024 * 1024)


def codes_of(amax):
    return jnp.ceil(CODES * jnp.log2(jnp.maximum(amax, 1e-30) * (1.0 / TOP))).astype(jnp.int32)


def scale_of(code):
    return jnp.exp2(code.astype(jnp.float32) * (1.0 / CODES))


def inverse_scale_of(code):
    return jnp.exp2(code.astype(jnp.float32) * (-1.0 / CODES))


def whole(x):
    return jnp.round(x).astype(jnp.int32)


def packed(low, high):
    return (low & 0xFFFF) | (high << 16)


def low_of(words):
    return (words << 16) >> 16


def high_of(words):
    return words >> 16


def column_of(head):
    return ((head >> 1) & 3) * 4 + (head >> 3)


def lanes():
    return lax.broadcasted_iota(jnp.int32, (8, LANES), 1)


def product_of(rows, weight):
    return lax.dot_general(
        weight, rows, (((1,), (1,)), ((), ())), preferred_element_type=jnp.float32
    )


def away_kernel(hidden, weight, out, my_rows, weight_rows, away_rows, arrived):
    core = lax.axis_index("core")
    odd = lax.axis_index("far")

    def rows_copy(l, x, other):
        first = pl.multiple_of((2 * x + (1 - core if other else core)) * SLICE, SLICE)
        target = away_rows if other else my_rows
        return pltpu.make_async_copy(
            hidden.at[l, pl.ds(first, SLICE), :],
            target.at[l, pl.ds(SLICE * x, SLICE), :],
            arrived.at[l, 2 * int(other) + x],
        )

    def weight_copies(l):
        blocks = pl.multiple_of(64 * odd, 64)
        half = pl.multiple_of(256 * (1 - odd), 64)
        return [
            pltpu.make_async_copy(
                weight.at[l, pl.ds(blocks, 256), :],
                weight_rows.at[l, pl.ds(0, 256), :],
                arrived.at[l, 4],
            ),
            pltpu.make_async_copy(
                weight.at[l, pl.ds(half, 64), :],
                weight_rows.at[l, pl.ds(256, 64), :],
                arrived.at[l, 5],
            ),
        ]

    for l in range(LAYERS):
        for copy in weight_copies(l):
            copy.start()
        for x in range(2):
            rows_copy(l, x, True).start()
    for l in range(EARLY):
        for x in range(2):
            rows_copy(l, x, False).start()

    @pl.loop(0, LAYERS)
    def _(l):
        for copy in weight_copies(l):
            copy.wait()
        for x in range(2):
            rows_copy(l, x, True).wait()
        value = product_of(away_rows[l], weight_rows[l])
        code = codes_of(jnp.max(jnp.abs(value), axis=0, keepdims=True))
        value = whole(value * inverse_scale_of(code))
        out[l, :LANES, :] = packed(value[:LANES], value[LANES : 2 * LANES])
        out[l, LANES:CODE_ROW, :] = packed(value[2 * LANES : 2 * LANES + 32], value[2 * LANES + 32 :])
        out[l, CODE_ROW:, :] = jnp.broadcast_to(code, (8, MINE))

    for l in range(EARLY):
        for x in range(2):
            rows_copy(l, x, False).wait()


def away_product(hidden, weight):
    return pl.pallas_call(
        away_kernel,
        in_specs=[HBM, HBM],
        out_specs=[VMEM, VMEM, VMEM],
        scratch_shapes=[
            pltpu.VMEM((LAYERS, MINE, DEPTH), jnp.bfloat16),
            pltpu.SemaphoreType.DMA((LAYERS, 6)),
        ],
        out_shape=[
            pltpu.VMEM((LAYERS, CODE_ROW + 8, MINE), jnp.int32),
            pltpu.VMEM((EARLY, MINE, DEPTH), jnp.bfloat16),
            pltpu.VMEM((LAYERS, WIDTH, DEPTH), jnp.bfloat16),
        ],
        cost_estimate=pl.CostEstimate(
            flops=LAYERS * MINE * DEPTH * WIDTH * 2, bytes_accessed=20_000_000, transcendentals=0
        ),
        compiler_params=limit(44),
        name="away_product",
    )(hidden, weight)


def my_kernel(
    hidden, rows, weight, src, grp, slot, out, src_out, grp_out, slot_out, late, arrived
):
    core = lax.axis_index("core")
    copies = []
    for x in range(2):
        first = pl.multiple_of((2 * x + core) * SLICE, SLICE)
        copies.append(
            pltpu.make_async_copy(
                hidden.at[EARLY, pl.ds(first, SLICE), :],
                late.at[pl.ds(SLICE * x, SLICE), :],
                arrived.at[x],
            )
        )
    for k, (here, there) in enumerate(((src, src_out), (grp, grp_out), (slot, slot_out))):
        copies.append(pltpu.make_async_copy(here, there, arrived.at[2 + k]))
    for copy in copies:
        copy.start()

    @pl.loop(0, EARLY)
    def _(l):
        out[l] = product_of(rows[l], weight[l])

    for copy in copies:
        copy.wait()
    out[EARLY] = product_of(late[...], weight[EARLY])


def my_product(hidden, rows, weight, src_block, group_map, q_slot):
    return pl.pallas_call(
        my_kernel,
        in_specs=[HBM, VMEM, VMEM, HBM, HBM, HBM],
        out_specs=[VMEM, SMEM, SMEM, SMEM],
        scratch_shapes=[
            pltpu.VMEM((MINE, DEPTH), jnp.bfloat16),
            pltpu.SemaphoreType.DMA((5,)),
        ],
        out_shape=[
            pltpu.VMEM((LAYERS, WIDTH, MINE), jnp.float32),
            pltpu.SMEM((KV_HEADS,), jnp.int32),
            pltpu.SMEM((KV_HEADS,), jnp.int32),
            pltpu.SMEM((KV_HEADS * GROUP,), jnp.int32),
        ],
        cost_estimate=pl.CostEstimate(
            flops=LAYERS * MINE * DEPTH * WIDTH * 2, bytes_accessed=12_000_000, transcendentals=0
        ),
        compiler_params=limit(24),
        name="my_product",
    )(hidden, rows, weight, src_block, group_map, q_slot)


TILES = LANES // 8


def pack_kernel(mine, theirs, out, sums):
    lane = lanes()
    odd = lax.axis_index("far")
    is_odd = odd == 1
    spare = (lane >= 64) != is_odd
    slot = lane & 63

    @pl.loop(0, 2, unroll=True)
    def _(x):
        codes = jnp.zeros((8, LANES), jnp.int32)
        first = x * (HEADS // 2)

        def place(head):
            return (head & 1) * HEADS + (head >> 1)

        for j in range(SLICE // LANES):
            tokens = pl.ds(pl.multiple_of(x * SLICE + j * LANES, LANES), LANES)

            top = None
            for l in range(LAYERS):
                scale = scale_of(theirs[l, CODE_ROW:, tokens])
                for at in range(0, CODE_ROW, 8):
                    word = theirs[l, at : at + 8, tokens]
                    low_row = at if at < LANES else at + LANES
                    high_row = low_row + (LANES if at < LANES else 32)
                    for row, half in ((low_row, low_of(word)), (high_row, high_of(word))):
                        value = mine[l, row : row + 8, tokens] + half.astype(jnp.float32) * scale
                        sums[l, row : row + 8, :] = value
                        value = jnp.abs(value)
                        top = value if top is None else jnp.maximum(top, value)
            code = codes_of(jnp.max(top, axis=0, keepdims=True))
            inverse = inverse_scale_of(code)
            rest = []
            for l in range(LAYERS):
                a = whole(sums[l, :LANES, :] * inverse)
                b = whole(sums[l, LANES : 2 * LANES, :] * inverse)
                words = packed(a, b).T.reshape(TILES, 8, LANES)
                for i in range(TILES):
                    out[first + place(j * TILES + i), 8 * l : 8 * l + 8, :] = words[i]
                rest.append(whole(sums[l, 2 * LANES :, :] * inverse))
            shown = jnp.broadcast_to(code, (64, LANES))
            low = jnp.concatenate(
                [jnp.where(is_odd, rest[1], rest[0]), jnp.where(is_odd, rest[0], rest[1])], axis=0
            )
            high = jnp.concatenate(
                [jnp.where(is_odd, shown, rest[2]), jnp.where(is_odd, rest[2], shown)], axis=0
            )
            words = packed(low, high).T.reshape(TILES, 8, LANES)
            for i in range(TILES):
                out[first + place(j * TILES + i), 24:32, :] = words[i]
                codes = jnp.where(slot == j * TILES + i, words[i], codes)
        codes = codes & ~0xFFFF
        shown = spare & (slot < HEADS)
        for i in range(HEADS):
            word = out[first + place(i), 24:32, :]
            out[first + place(i), 24:32, :] = jnp.where(shown, (word & 0xFFFF) | codes, word)


def pack(mine, theirs):
    return pl.pallas_call(
        pack_kernel,
        in_specs=[VMEM, VMEM],
        out_specs=VMEM,
        scratch_shapes=[pltpu.VMEM((LAYERS, WIDTH, LANES), jnp.float32)],
        out_shape=pltpu.VMEM((2 * HEADS, 32, LANES), jnp.int32),
        compiler_params=limit(16),
        name="pack",
    )(mine, theirs)


def device_of(source, x, m):
    return (m & 1) * HEADS + x * (HEADS // 2) + source + (m >> 1)


def reached(scale):
    halves = []
    for x in range(2):
        top = scale[x, 0]
        for m in range(1, GROUP_DEVS):
            top = jnp.maximum(top, scale[x, m])
        halves.append(top)
    return halves[0] + halves[1]


def route_kernel(src, grp, slot, words, out, scales, whole_q, where_q):
    left = lanes() < 64

    @pl.loop(0, KV_HEADS, unroll=True)
    def _(r):
        source = src[r] * (GROUP_DEVS // 2)
        target = column_of(grp[r] * GROUP_DEVS)
        for j in range(GROUP):
            where_q[slot[r * GROUP + j]] = j
        scale = {}
        for x in range(2):
            for m in range(GROUP_DEVS):
                code = high_of(words[device_of(source, x, m), 24:32, :])
                at = 96 if m % 2 == 0 else 32
                scale[x, m] = scale_of(code[:, at : at + 1])
        inverse = 1.0 / reached(scale)
        blocks = [[None] * 10 for _ in range(LAYERS)]
        for pair in range(2):
            even, odd = 2 * pair, 2 * pair + 1
            tiles = {}
            rest = None
            for x in range(2):
                third = {}
                for m in (even, odd):
                    device = device_of(source, x, m)
                    last = words[device, 24:32, :]
                    low, high = low_of(last), high_of(last)
                    ratio = scale[x, m] * inverse
                    third[m] = (low.astype(jnp.float32) * ratio, high.astype(jnp.float32) * ratio)
                    for l in range(LAYERS):
                        word = words[device, 8 * l : 8 * l + 8, :]
                        a = low_of(word).astype(jnp.float32) * ratio
                        b = high_of(word).astype(jnp.float32) * ratio
                        if x == 0:
                            tiles[m, l] = (a, b)
                        else:
                            tiles[m, l] = (tiles[m, l][0] + a, tiles[m, l][1] + b)
                part = [
                    jnp.where(left, third[even][0], third[odd][0]),
                    jnp.where(left, third[odd][0], third[even][0]),
                    jnp.where(left, third[even][1], third[odd][1]),
                ]
                rest = part if x == 0 else [p + q for p, q in zip(rest, part)]
            rest[1] = pltpu.roll(rest[1], 64, 1)
            for l in range(LAYERS):
                blocks[l][5 * pair : 5 * pair + 5] = [
                    tiles[even, l][0],
                    tiles[even, l][1],
                    rest[l],
                    tiles[odd, l][0],
                    tiles[odd, l][1],
                ]
        for l in range(LAYERS):
            for j in range(GROUP):
                whole_q[j, l] = whole(blocks[l][j])
            key_value = packed(whole(blocks[l][8]), whole(blocks[l][9]))
            for s in range(GROUP_DEVS):
                device = target + (s & 1) * (HEADS // 2) + column_of(s)
                out[device, 24 + 8 * l : 32 + 8 * l, :] = key_value
        for s in range(GROUP_DEVS):
            device = target + (s & 1) * (HEADS // 2) + column_of(s)
            first, second = where_q[2 * s] & 7, where_q[2 * s + 1] & 7
            for l in range(LAYERS):
                out[device, 8 * l : 8 * l + 8, :] = packed(whole_q[first, l], whole_q[second, l])

    own = lax.axis_index("z") * 2 + (lax.axis_index("y") >> 1)
    block = 0
    for r in range(KV_HEADS):
        block = jnp.where(grp[r] == own, src[r], block)
    source = block * (GROUP_DEVS // 2)
    scale = {}
    for x in range(2):
        for m in range(GROUP_DEVS):
            code = high_of(words[device_of(source, x, m), 24:32, :])
            code = code if m % 2 == 0 else pltpu.roll(code, 64, 1)
            scale[x, m] = scale_of(code)
    scales[...] = reached(scale)


def route(src, grp, slot, words):
    return pl.pallas_call(
        route_kernel,
        in_specs=[SMEM, SMEM, SMEM, VMEM],
        out_specs=[VMEM, VMEM],
        scratch_shapes=[
            pltpu.VMEM((GROUP, LAYERS, 8, LANES), jnp.int32),
            pltpu.SMEM((GROUP,), jnp.int32),
        ],
        out_shape=[
            pltpu.VMEM((HEADS, 48, LANES), jnp.int32),
            pltpu.VMEM((8, LANES), jnp.float32),
        ],
        compiler_params=limit(16),
        name="route",
    )(src, grp, slot, words)


OPEN_HEADS = 16


def open_kernel(words, scales, out):
    step = pl.program_id(0)
    scale_columns = pltpu.roll(scales[...], 64 - OPEN_HEADS * step, 1)
    for i in range(OPEN_HEADS):
        block = (i & 1) * (HEADS // 2) + column_of(i) + step * (OPEN_HEADS // 8)
        scale = scale_columns[:, i : i + 1]
        rows = slice(8 * i, 8 * i + 8)
        for l in range(LAYERS):
            for half in range(2):
                first = 24 * half + 8 * l
                word = words[block, first : first + 8, :]
                cols = 2 * LANES * half
                out[l, rows, cols : cols + LANES] = low_of(word).astype(jnp.float32) * scale
                out[l, rows, cols + LANES : cols + 2 * LANES] = (
                    high_of(word).astype(jnp.float32) * scale
                )


def opened(words, scales):
    return pl.pallas_call(
        open_kernel,
        grid=(HEADS // OPEN_HEADS,),
        in_specs=[VMEM, VMEM],
        out_specs=pl.BlockSpec((LAYERS, 8 * OPEN_HEADS, 4 * LANES), lambda h: (0, h, 0)),
        out_shape=jax.ShapeDtypeStruct((LAYERS, SLICE, 4 * LANES), jnp.float32),
        compiler_params=limit(16),
        name="opened",
    )(words, scales)


def on_device(hidden, joined_weight, src_block, group_map, q_slot):
    hidden = pltpu.with_memory_space_constraint(hidden, pltpu.HBM)
    weight = pltpu.with_memory_space_constraint(jnp.swapaxes(joined_weight, 1, 2), pltpu.HBM)
    away, rows, weight = away_product(hidden, weight)
    theirs = lax.ppermute(away, "core", [(0, 1), (1, 0)])
    tables = [pltpu.with_memory_space_constraint(t, pltpu.HBM) for t in (src_block, group_map, q_slot)]
    mine, *tables = my_product(hidden, rows, weight, *tables)
    words = pack(mine, theirs)
    words = lax.all_to_all(words, ("far", "near", "z", "y"), 0, 0, tiled=True)
    words, scales = route(*tables, words)
    words = lax.all_to_all(words, ("far", "y", "z"), 0, 0, tiled=True)
    return opened(words, scales)


def solution(mesh):
    split = Mesh(mesh.devices.reshape(4, 4, 2, 2, 2), ("z", "y", "far", "near", "core"))
    head, kdim = ("z", "y", "far"), ("near", "core")
    return jax.shard_map(
        on_device,
        mesh=split,
        in_specs=(P(None, None, kdim), P(None, kdim, head), P(), P(), P()),
        out_specs=P(None, kdim, head),
        check_vma=False,
    )
```
